256 devices in a mesh: gx: 32 (over z, x_hi, core), gy: 8 (over x_lo, y).
Axes of the slice: x: 4 (x_hi: 2, x_lo: 2; x = x_hi * 2 + x_lo), y: 4, z: 8, core: 2. Of those that a mesh axis runs over, the one named last changes fastest.
Arguments:
- positions: float32 [3, 12, 64, 128, 256], P(None, None, 'gx', 'gy'), may hold values from 0 to 1
- velocities: float32 [3, 12, 64, 128, 256], P(None, None, 'gx', 'gy'), may hold values from -6 to 6
- thermal: float32 [3, 12, 64, 128, 256], P(None, None, 'gx', 'gy'), may hold values from -6 to 6
- offsets: int32 [12, 64, 128, 256], P(None, 'gx', 'gy'), may hold values from 0 to 7
- occupancy: int32 [12, 64, 128, 256], P(None, 'gx', 'gy'), may hold values from 0 to 1, as said below
- shift_codes: int32 [3], replicated, may hold values from 0 to 7
Outputs:
- new_velocities: float32 [3, 12, 64, 128, 256], P(None, None, 'gx', 'gy')
The draws below stay inside these ranges and needn't reach their ends.
Inputs may be any that keep to these rules, and one draw needn't show every extreme that they name: `occupancy`: the particles of a storage cell occupy its first slots; every storage cell holds 8 to 12 particles.
All inputs are finite; a program needn't handle non-finite values.
Results may differ from the reference program's by a relative error of at most 0.0001.
Values sent between devices are 32-bit elements; how exact they have to be, the bound alone decides.
No kernel may reach another device: no remote copies, remote signals or barrier semaphores. Data moves between devices by JAX's collectives and lax.ppermute only.
A program may use at most 64 MiB of HBM per device.

```python
import jax
import jax.numpy as jnp

CZ = 256
SLOTS = 12
STEPS = 3
NX = 64
NY = 128


def draw_occupancy(key, part):
    counts = jax.random.randint(key, (1, NX, NY, CZ), SLOTS - 4, SLOTS + 1)
    slot_ids = jnp.arange(SLOTS, dtype=jnp.int32).reshape(SLOTS, 1, 1, 1)
    return (slot_ids < counts).astype(jnp.int32)


def touch_ends(drawn, own_key, least, largest):
    longest = drawn.shape.index(max(drawn.shape))
    spots = []
    for shift in (0, 1):
        where = [jax.random.randint(jax.random.fold_in(own_key, axis), (), 0, length) for axis, length in enumerate(drawn.shape)]
        where[longest] = (where[longest] + shift) % drawn.shape[longest]
        spots.append(tuple(where))
    return drawn.at[spots[0]].set(least).at[spots[1]].set(largest)


def levels(key, shape, cuts, least, largest):
    gain = 1.0
    for axis_at, blocks in cuts:
        draws = jax.random.uniform(jax.random.fold_in(jax.random.fold_in(key, 6), axis_at), (blocks,), jnp.float32, least / len(cuts), largest / len(cuts))
        gain = gain * jnp.repeat(jnp.exp(draws), shape[axis_at] // blocks).reshape((-1,) + (1,) * (len(shape) - 1 - axis_at))
    return gain


def bell_draw(own_key, extent, scale, reach, cuts=(), kind=jnp.bfloat16):
    gain = levels(own_key, extent, cuts, -0.22, 0.18) if cuts else 1.0
    drawn = jax.random.normal(own_key, extent, jnp.float32) * scale * gain
    return jnp.minimum(jnp.maximum(drawn, -reach), reach).astype(kind)


def setup_inputs(seed: int = 0) -> dict:
    splits = jax.random.split(jax.random.key(seed), 7)
    positions = jnp.clip(1.0 * jax.random.uniform(splits[0], (3, SLOTS, NX, NY, CZ), jnp.float32) ** levels(splits[0], (3, SLOTS, NX, NY, CZ), ((2, 32), (3, 8)), -0.2, 0.2), 0.0, 1.0)
    velocities = bell_draw(splits[1], (3, SLOTS, NX, NY, CZ), 1.0, 6.0, ((2, 32), (3, 8)), jnp.float32)
    thermal = bell_draw(splits[2], (3, SLOTS, NX, NY, CZ), 1.0, 6.0, ((2, 32), (3, 8)), jnp.float32)
    offsets = touch_ends(jax.random.randint(splits[3], (SLOTS, NX, NY, CZ), 0, 8), jax.random.fold_in(splits[3], 1), 0, 7).astype(jnp.int32)
    occupancy = draw_occupancy(jax.random.fold_in(splits[6], 71), 0)
    shift_codes = jax.random.randint(splits[5], (STEPS,), 0, 8).astype(jnp.int32)
    return dict(positions=positions, velocities=velocities, thermal=thermal, offsets=offsets, occupancy=occupancy, shift_codes=shift_codes)


ridge = 0.5


def offset_bits(code_value):
    return code_value // 4, (code_value // 2) % 2, code_value % 2


def cross_product(first, second):
    return [first[1] * second[2] - first[2] * second[1],
            first[2] * second[0] - first[0] * second[2],
            first[0] * second[1] - first[1] * second[0]]


def code_moments(positions, velocities, thermal, offsets, occupancy, code_value):
    shift_x, shift_y, shift_z = offset_bits(code_value)
    weight = jnp.where(offsets == code_value, occupancy, 0).astype(jnp.float32)
    shifted = [positions[0] + shift_x, positions[1] + shift_y, positions[2] + shift_z]
    relative = [velocities[component] - thermal[component] for component in range(3)]
    spins = cross_product(shifted, relative)
    seconds = [shifted[0] * shifted[0], shifted[1] * shifted[1], shifted[2] * shifted[2],
               shifted[0] * shifted[1], shifted[0] * shifted[2], shifted[1] * shifted[2]]
    terms = shifted + relative + spins + seconds
    return jnp.stack([jnp.sum(weight, axis=0)] + [jnp.sum(weight * term, axis=0) for term in terms])


def cell_solution(sums):
    count = jnp.maximum(sums[0], 1.0)
    first = [sums[1], sums[2], sums[3]]
    flow = [sums[4], sums[5], sums[6]]
    centre = [value / count for value in first]
    drift = [value / count for value in flow]
    moment = cross_product(centre, flow)
    torque = [sums[7 + component] - moment[component] for component in range(3)]
    mxx = sums[10] - first[0] * first[0] / count
    myy = sums[11] - first[1] * first[1] / count
    mzz = sums[12] - first[2] * first[2] / count
    mxy = sums[13] - first[0] * first[1] / count
    mxz = sums[14] - first[0] * first[2] / count
    myz = sums[15] - first[1] * first[2] / count
    trace = mxx + myy + mzz
    kxx = trace - mxx + ridge
    kyy = trace - myy + ridge
    kzz = trace - mzz + ridge
    kxy = -mxy
    kxz = -mxz
    kyz = -myz
    adj_xx = kyy * kzz - kyz * kyz
    adj_yy = kxx * kzz - kxz * kxz
    adj_zz = kxx * kyy - kxy * kxy
    adj_xy = kxz * kyz - kxy * kzz
    adj_xz = kxy * kyz - kxz * kyy
    adj_yz = kxy * kxz - kxx * kyz
    determinant = kxx * adj_xx + kxy * adj_xy + kxz * adj_xz
    spin_x = (adj_xx * torque[0] + adj_xy * torque[1] + adj_xz * torque[2]) / determinant
    spin_y = (adj_xy * torque[0] + adj_yy * torque[1] + adj_yz * torque[2]) / determinant
    spin_z = (adj_xz * torque[0] + adj_yz * torque[1] + adj_zz * torque[2]) / determinant
    return jnp.stack(centre + drift + [spin_x, spin_y, spin_z])


def particle_update(table, positions, thermal, offsets, occupancy, code_value, total):
    shift_x, shift_y, shift_z = offset_bits(code_value)
    shifted = [positions[0] + shift_x, positions[1] + shift_y, positions[2] + shift_z]
    arm = [shifted[component] - table[component] for component in range(3)]
    turn = cross_product([table[6], table[7], table[8]], arm)
    fresh = jnp.stack([thermal[component] + table[3 + component] + turn[component] for component in range(3)])
    keep = (offsets == code_value) & (occupancy == 1)
    return total + jnp.where(keep, fresh, jnp.zeros_like(fresh))


def one_collision(positions, velocities, thermal, offsets, occupancy):
    cell_sums = jnp.zeros((16,) + offsets.shape[1:], jnp.float32)
    for code_value in range(8):
        shift_x, shift_y, shift_z = offset_bits(code_value)
        partial_sums = code_moments(positions, velocities, thermal, offsets, occupancy, code_value)
        cell_sums = cell_sums + jnp.roll(partial_sums, (-shift_x, -shift_y, -shift_z), axis=(1, 2, 3))
    state = cell_solution(cell_sums)
    result = jnp.zeros(positions.shape, jnp.float32)
    for code_value in range(8):
        shift_x, shift_y, shift_z = offset_bits(code_value)
        table = jnp.roll(state, (shift_x, shift_y, shift_z), axis=(1, 2, 3))
        result = particle_update(table, positions, thermal, offsets, occupancy, code_value, result)
    return result


def reference(positions, velocities, thermal, offsets, occupancy, shift_codes):
    current = velocities
    for step_index in range(STEPS):
        codes = jnp.bitwise_xor(offsets, shift_codes[step_index])
        hot = jnp.roll(thermal, -step_index, axis=1)
        current = one_collision(positions, current, hot, codes, occupancy)
    return current
```

```python
import functools

import jax
import jax.numpy as jnp
from jax import lax
from jax.experimental import pallas as pl
from jax.experimental.pallas import tpu as pltpu
from jax.sharding import PartitionSpec as P

STEPS = 3
RIDGE = 0.5
GROUPS = 8
F32 = jnp.float32


def bits(code):
    return code // 4, code // 2 % 2, code % 2


def cross(u, v):
    return [
        u[1] * v[2] - u[2] * v[1],
        u[2] * v[0] - u[0] * v[2],
        u[0] * v[1] - u[1] * v[0],
    ]


def plus(terms):
    total = None
    for term in terms:
        total = term if total is None else total + term
    return total


def accumulate(value_ref, code_ref, count, out_ref, lanes, start, per_block, with_count):
    slots = code_ref.shape[0]
    names = (["n"] if with_count else []) + list(range(count))
    for first in range(0, len(names), per_block):
        block = names[first : first + per_block]
        for base in (0, 4):
            sums = [[None] * 4 for _ in block]
            for slot in range(slots):
                code = code_ref[slot]
                masks = [code == base + g for g in range(4)]
                for at, name in enumerate(block):
                    for g in range(4):
                        if name == "n":
                            part = jnp.where(masks[g], 1.0, 0.0)
                        else:
                            part = jnp.where(masks[g], value_ref[name, slot], 0.0)
                        old = sums[at][g]
                        sums[at][g] = part if old is None else old + part
            for at in range(len(block)):
                for g in range(4):
                    out_ref[base + g, start + first + at, 0, :, lanes] = sums[at][g]


def store_codes(offsets, occupancy, code_ref, lanes):
    for slot in range(offsets.shape[0]):
        code_ref[slot] = jnp.where(
            occupancy[slot, 0, :, lanes] == 1, offsets[slot, 0, :, lanes], GROUPS
        )


def first_sums_kernel(pos, vel, thermal, offsets, occupancy, geo, wsum, value_ref, code_ref):
    slots = offsets.shape[0]
    for half in range(pos.shape[4] // 128):
        lanes = pl.ds(half * 128, 128)
        store_codes(offsets, occupancy, code_ref, lanes)
        for slot in range(slots):
            p = [pos[c, slot, 0, :, lanes] for c in range(3)]
            w = [vel[c, slot, 0, :, lanes] - thermal[c, slot, 0, :, lanes] for c in range(3)]
            seconds = [p[0] * p[0], p[1] * p[1], p[2] * p[2], p[0] * p[1], p[0] * p[2], p[1] * p[2]]
            for at, value in enumerate(p + seconds + w + cross(p, w)):
                value_ref[at, slot] = value
        accumulate(value_ref, code_ref, 9, geo, lanes, 0, 5, True)
        accumulate(value_ref.at[pl.ds(9, 6)], code_ref, 6, wsum, lanes, 0, 6, False)


def later_sums_kernel(pos, thermal, offsets, occupancy, dsum1, dsum2, value_ref, code_ref):
    slots = offsets.shape[0]
    for half in range(pos.shape[4] // 128):
        lanes = pl.ds(half * 128, 128)
        store_codes(offsets, occupancy, code_ref, lanes)
        for slot in range(slots):
            p = [pos[c, slot, 0, :, lanes] for c in range(3)]
            hot = [
                [thermal[c, (slot + s) % slots, 0, :, lanes] for c in range(3)] for s in range(3)
            ]
            for s in range(2):
                d = [hot[s][c] - hot[s + 1][c] for c in range(3)]
                for at, value in enumerate(d + cross(p, d)):
                    value_ref[6 * s + at, slot] = value
        accumulate(value_ref.at[pl.ds(0, 6)], code_ref, 6, dsum1, lanes, 0, 6, False)
        accumulate(value_ref.at[pl.ds(6, 6)], code_ref, 6, dsum2, lanes, 0, 6, False)


def roll(value, amount):
    return pltpu.roll(value, amount % value.shape[-1], value.ndim - 1)


def frame_sums(geo, wsum, o, code, row):
    bx, by, bz = bits(code)
    n = geo[o, 0, row]
    s = [geo[o, 1 + c, row] for c in range(3)]
    m = [geo[o, 4 + c, row] for c in range(6)]
    w = [wsum[o, c, row] for c in range(3)]
    l = [wsum[o, 3 + c, row] for c in range(3)]
    b = (bx, by, bz)
    q = [s[c] + n if b[c] else s[c] for c in range(3)]
    qq = []
    for at, (i, j) in enumerate(((0, 0), (1, 1), (2, 2), (0, 1), (0, 2), (1, 2))):
        value = m[at]
        if b[i]:
            value = value + s[j]
        if b[j]:
            value = value + q[i]
        qq.append(value)
    if bx:
        l = [l[0], l[1] - w[2], l[2] + w[1]]
    if by:
        l = [l[0] + w[2], l[1], l[2] - w[0]]
    if bz:
        l = [l[0] - w[1], l[1] + w[0], l[2]]
    return [n] + q + w + l + qq


def expand(geo, wsum, shift, rows, yup, ydn, part, shifted):
    cols = geo.shape[3]
    shifted[cols:, :] = jnp.zeros_like(shifted[cols:, :])
    for by in range(2):
        for bz in range(2):
            low = 2 * by + bz
            for bx in range(2):
                code = 4 * bx + low
                o = code ^ shift
                for row in range(2):
                    values = frame_sums(geo, wsum, o, code, row)
                    for v in range(16):
                        if bx == 1 and row == 1:
                            part[by, bz, 1, v] += values[v]
                        else:
                            part[by, bz, row + 1 - bx, v] = values[v]
    for r in range(3):
        for v in range(16):
            near = part[0, 0, r, v] + roll(part[0, 1, r, v], -1)
            beyond = part[1, 0, r, v] + roll(part[1, 1, r, v], -1)
            shifted[:cols, :] = beyond
            main = near + shifted[1 : cols + 1, :]
            rows[r][v] = main
            rows[r][16, v : v + 1, :] = beyond[0:1]
            yup[r, v : v + 1, :] = main[cols - 1 : cols]
            ydn[r, v : v + 1, :] = beyond[0:1]


def expand_kernel(codes, geo, wsum, row0, row1, row2, yup, ydn, part, shifted):
    expand(geo, wsum, codes[0], (row0, row1, row2), yup, ydn, part, shifted)


def fold_row(row, r, yprev, ynext, out):
    last = row.shape[1] - 1
    out[...] = row[...]
    out[16] = row[16] + yprev[r]
    for v in range(16):
        out[v, last : last + 1, :] = row[v, last : last + 1, :] + ynext[r, v : v + 1, :]


def fold_kernel(row0, row2, yprev, ynext, out0, out2):
    fold_row(row0, 0, yprev, ynext, out0)
    fold_row(row2, 2, yprev, ynext, out2)


def solve(sums):
    inverse = 1.0 / jnp.maximum(sums[0], 1.0)
    first = sums[1:4]
    flow = sums[4:7]
    centre = [value * inverse for value in first]
    drift = [value * inverse for value in flow]
    moment = cross(centre, flow)
    torque = [sums[7 + c] - moment[c] for c in range(3)]
    mxx = sums[10] - first[0] * centre[0]
    myy = sums[11] - first[1] * centre[1]
    mzz = sums[12] - first[2] * centre[2]
    kxy = first[0] * centre[1] - sums[13]
    kxz = first[0] * centre[2] - sums[14]
    kyz = first[1] * centre[2] - sums[15]
    kxx = myy + mzz + RIDGE
    kyy = mxx + mzz + RIDGE
    kzz = mxx + myy + RIDGE
    adj_xx = kyy * kzz - kyz * kyz
    adj_yy = kxx * kzz - kxz * kxz
    adj_zz = kxx * kyy - kxy * kxy
    adj_xy = kxz * kyz - kxy * kzz
    adj_xz = kxy * kyz - kxz * kyy
    adj_yz = kxy * kxz - kxx * kyz
    scale = 1.0 / (kxx * adj_xx + kxy * adj_xy + kxz * adj_xz)
    spin = [
        (adj_xx * torque[0] + adj_xy * torque[1] + adj_xz * torque[2]) * scale,
        (adj_xy * torque[0] + adj_yy * torque[1] + adj_yz * torque[2]) * scale,
        (adj_xz * torque[0] + adj_yz * torque[1] + adj_zz * torque[2]) * scale,
    ]
    turned = cross(spin, centre)
    return [drift[c] - turned[c] for c in range(3)] + spin


def fill_table(own0, row1, own2, yprev, ynext, xprev, xnext, total, table):
    cols = row1.shape[1]
    fold_row(row1, 1, yprev, ynext, total)
    for r in range(3):
        if r == 0:
            read = lambda v, at: own0[v, at, :] + xprev[v, at, :]
        elif r == 1:
            read = lambda v, at: total[v, at, :]
        else:
            read = lambda v, at: own2[v, at, :] + xnext[v, at, :]
        for t in range(cols // 8):
            state = solve([read(v, pl.ds(8 * t, 8)) for v in range(16)])
            for v in range(6):
                table[0, v, r, 8 + 8 * t : 16 + 8 * t, :] = state[v]
                table[1, v, r, 8 + 8 * t : 16 + 8 * t, :] = roll(state[v], 1)
        state = solve([read(16, pl.ds(v, 1)) for v in range(16)])
        for v in range(6):
            wide = jnp.broadcast_to(state[v], (8, state[v].shape[1]))
            table[0, v, r, 0:8, :] = wide
            table[1, v, r, 0:8, :] = roll(wide, 1)


def shift_a(a, spin, b):
    a = list(a)
    if b[0]:
        a = [a[0], a[1] + spin[2], a[2] - spin[1]]
    if b[1]:
        a = [a[0] - spin[2], a[1], a[2] + spin[0]]
    if b[2]:
        a = [a[0] + spin[1], a[1] - spin[0], a[2]]
    return a


def update_groups(geo, dsum, shift, table, wsum):
    cols = geo.shape[3]
    for code in range(GROUPS):
        bx, by, bz = bits(code)
        o = code ^ shift
        for row in range(2):
            for t in range(cols // 8):
                at = pl.ds(8 * t, 8)
                from_col = 8 + 8 * t - by
                values = [table[bz, v, row + 1 - bx, from_col : from_col + 8, :] for v in range(6)]
                spin = values[3:]
                a = shift_a(values[:3], spin, (bx, by, bz))
                n = geo[o, 0, row, at, :]
                s = [geo[o, 1 + c, row, at, :] for c in range(3)]
                xx, yy, zz, xy, xz, yz = [geo[o, 4 + c, row, at, :] for c in range(6)]
                turn = cross(spin, s)
                arm = cross(s, a)
                own = [
                    (yy + zz) * spin[0] - xy * spin[1] - xz * spin[2],
                    (xx + zz) * spin[1] - xy * spin[0] - yz * spin[2],
                    (xx + yy) * spin[2] - xz * spin[0] - yz * spin[1],
                ]
                for c in range(3):
                    wsum[o, c, row, at, :] = dsum[o, c, row, at, :] + n * a[c] + turn[c]
                    wsum[o, 3 + c, row, at, :] = dsum[o, 3 + c, row, at, :] + arm[c] + own[c]


def step_kernel(
    codes, geo, dsum, own0, mid, own2, yprev, ynext, xprev, xnext,
    row0, row1, row2, yup, ydn, total, table, wsum, part, shifted,
):
    fill_table(own0, mid, own2, yprev, ynext, xprev, xnext, total, table)
    update_groups(geo, dsum, codes[0], table, wsum)
    expand(geo, wsum, codes[1], (row0, row1, row2), yup, ydn, part, shifted)


def last_kernel(own0, mid, own2, yprev, ynext, xprev, xnext, table, total):
    fill_table(own0, mid, own2, yprev, ynext, xprev, xnext, total, table)


def pick(mask, yes, no):
    return [jnp.where(mask, y, n) for y, n in zip(yes, no)]


def particles_kernel(codes, table, pos, thermal, offsets, occupancy, out, variants):
    slots = offsets.shape[0]
    row = pl.program_id(0)
    tile = pl.program_id(1)
    for half in range(pos.shape[4] // 128):
        lanes = pl.ds(half * 128, 128)
        for code in range(GROUPS):
            bx, by, bz = bits(code)
            values = [
                table[bz, v, row + 1 - bx, pl.ds(8 * tile, 16), lanes][8 - by : 16 - by]
                for v in range(6)
            ]
            values[:3] = shift_a(values[:3], values[3:], (bx, by, bz))
            for v in range(6):
                variants[code, v] = values[v]
        for slot in range(slots):
            k = offsets[slot, 0, :, lanes] ^ codes[0]
            isx, isy, isz = (k & 4) != 0, (k & 2) != 0, (k & 1) != 0
            used = occupancy[slot, 0, :, lanes] == 1
            state = []
            for v in range(6):
                level = [jnp.where(isx, variants[4 + i, v], variants[i, v]) for i in range(4)]
                level = [jnp.where(isy, level[2 + i], level[i]) for i in range(2)]
                state.append(jnp.where(isz, level[1], level[0]))
            p = [pos[c, slot, 0, :, lanes] for c in range(3)]
            turn = cross(state[3:], p)
            for c in range(3):
                fresh = thermal[c, (slot + STEPS - 1) % slots, 0, :, lanes] + (state[c] + turn[c])
                out[c, slot, 0, :, lanes] = jnp.where(used, fresh, 0.0)


VMEM = pl.BlockSpec(memory_space=pltpu.VMEM)
SMEM = pl.BlockSpec(memory_space=pltpu.SMEM)


def shape(*dims):
    return jax.ShapeDtypeStruct(dims, F32)


def big_spec(lead):
    return pl.BlockSpec((*lead, 1, 8, 256), lambda r, t: (*([0] * len(lead)), r, t, 0))


def local(positions, velocities, thermal, offsets, occupancy, shift_codes):
    slots, rows, cols, depth = offsets.shape
    grid = (rows, cols // 8)
    vec = big_spec((3, slots))
    flat = big_spec((slots,))
    group = lambda count: pltpu.VMEM((GROUPS, count, rows, cols, depth), F32)
    group_shape = lambda count: shape(GROUPS, count, rows, cols, depth)
    group_spec = lambda count: big_spec((GROUPS, count))
    scratch = lambda count: [
        pltpu.VMEM((count, slots, 8, 128), F32),
        pltpu.VMEM((slots, 8, 128), jnp.int32),
    ]

    geo, wsum = pl.pallas_call(
        first_sums_kernel,
        grid=grid,
        in_specs=[vec, vec, vec, flat, flat],
        out_specs=[group_spec(10), group_spec(6)],
        out_shape=[group_shape(10), group_shape(6)],
        scratch_shapes=scratch(15),
        name="first_sums",
    )(positions, velocities, thermal, offsets, occupancy)

    row_shape = shape(17, cols, depth)
    col_shape = shape(3, 16, depth)
    expand_out = [row_shape] * 3 + [col_shape] * 2
    expand_scratch = [
        pltpu.VMEM((2, 2, 3, 16, cols, depth), F32),
        pltpu.VMEM((cols + 8, depth), F32),
    ]
    total = pltpu.VMEM((17, cols, depth), F32)
    table_shape = (2, 6, 3, cols + 8, depth)

    row0, row1, row2, yup, ydn = pl.pallas_call(
        expand_kernel,
        in_specs=[SMEM, VMEM, VMEM],
        out_specs=[VMEM] * 5,
        out_shape=expand_out,
        scratch_shapes=expand_scratch,
        name="expand",
    )(shift_codes[0:1], geo, wsum)

    def ring(axis, by):
        count = lax.axis_size(axis)
        return [(i, (i + by) % count) for i in range(count)]

    dsums = None
    for step in range(STEPS):
        yprev = lax.ppermute(yup, "gy", ring("gy", 1))
        ynext = lax.ppermute(ydn, "gy", ring("gy", -1))
        if dsums is None:
            dsums = pl.pallas_call(
                later_sums_kernel,
                grid=grid,
                in_specs=[vec, vec, flat, flat],
                out_specs=[group_spec(6), group_spec(6)],
                out_shape=[group_shape(6), group_shape(6)],
                scratch_shapes=scratch(12),
                name="later_sums",
            )(positions, thermal, offsets, occupancy)
        own0, own2 = pl.pallas_call(
            fold_kernel,
            in_specs=[VMEM] * 4,
            out_specs=[VMEM] * 2,
            out_shape=[row_shape] * 2,
            name="fold",
        )(row0, row2, yprev, ynext)
        xprev = lax.ppermute(own2, "gx", ring("gx", 1))
        xnext = lax.ppermute(own0, "gx", ring("gx", -1))
        if step + 1 < STEPS:
            row0, row1, row2, yup, ydn = pl.pallas_call(
                step_kernel,
                in_specs=[SMEM] + [VMEM] * 9,
                out_specs=[VMEM] * 5,
                out_shape=expand_out,
                scratch_shapes=[total, pltpu.VMEM(table_shape, F32), group(6)] + expand_scratch,
                name="step",
            )(shift_codes[step : step + 2], geo, dsums[step], own0, row1, own2, yprev, ynext, xprev, xnext)

    table = pl.pallas_call(
        last_kernel,
        in_specs=[VMEM] * 7,
        out_specs=VMEM,
        out_shape=shape(*table_shape),
        scratch_shapes=[total],
        name="last",
    )(own0, row1, own2, yprev, ynext, xprev, xnext)

    return pl.pallas_call(
        particles_kernel,
        grid=grid,
        in_specs=[SMEM, VMEM, vec, vec, flat, flat],
        out_specs=vec,
        out_shape=shape(3, slots, rows, cols, depth),
        scratch_shapes=[pltpu.VMEM((GROUPS, 6, 8, 128), F32)],
        name="particles",
    )(shift_codes[STEPS - 1 : STEPS], table, positions, thermal, offsets, occupancy)


def solution(mesh):
    in_specs = (
        P(None, None, "gx", "gy", None),
        P(None, None, "gx", "gy", None),
        P(None, None, "gx", "gy", None),
        P(None, "gx", "gy", None),
        P(None, "gx", "gy", None),
        P(),
    )
    out_specs = P(None, None, "gx", "gy", None)
    return jax.shard_map(local, mesh=mesh, in_specs=in_specs, out_specs=out_specs, check_vma=False)
```

```python
import functools

import jax
import jax.numpy as jnp
from jax import lax
from jax.experimental import pallas as pl
from jax.experimental.pallas import tpu as pltpu
from jax.sharding import PartitionSpec as P


STEPS = 3
RIDGE = 0.5
GROUPS = 8
F32 = jnp.float32


def bits(code):
    return code // 4, code // 2 % 2, code % 2


def cross(u, v):
    return [
        u[1] * v[2] - u[2] * v[1],
        u[2] * v[0] - u[0] * v[2],
        u[0] * v[1] - u[1] * v[0],
    ]


def plus(terms):
    total = None
    for term in terms:
        total = term if total is None else total + term
    return total


def accumulate(value_ref, codes, groups, names, store):
    sums = [[None] * len(groups) for _ in names]
    for slot, code in enumerate(codes):
        masks = [code == group for group in groups]
        for at, name in enumerate(names):
            value = 1.0 if name is None else value_ref[name, slot]
            for g, mask in enumerate(masks):
                part = jnp.where(mask, value, 0.0)
                old = sums[at][g]
                sums[at][g] = part if old is None else old + part
    for at in range(len(names)):
        for g in range(len(groups)):
            store(at, g, sums[at][g])


def moments(p, w):
    seconds = [p[0] * p[0], p[1] * p[1], p[2] * p[2], p[0] * p[1], p[0] * p[2], p[1] * p[2]]
    return p + seconds + w + cross(p, w)


def chunk_sums(pos, rel, code, value, geo, wsum, groups, row, at, lanes):
    slots = code.shape[0]
    for slot in range(slots):
        p = [pos[c, slot, row, at, lanes] for c in range(3)]
        w = [rel[c, slot, row, at, lanes] for c in range(3)]
        for name, term in enumerate(moments(p, w)):
            value[name, slot] = term
    codes = [code[slot, row, at, lanes] for slot in range(slots)]

    def store_first(index, g, total):
        geo[groups[g], index, row, at, lanes] = total

    def store_second(index, g, total):
        if index < 2:
            geo[groups[g], 8 + index, row, at, lanes] = total
        else:
            wsum[groups[g], index - 2, row, at, lanes] = total

    accumulate(value, codes, groups, [None] + list(range(7)), store_first)
    accumulate(value, codes, groups, list(range(7, 15)), store_second)


def halves(depth):
    return [pl.ds(128 * half, 128) for half in range(depth // 128)]


def four(by, shift):
    return [(4 * bx + 2 * by + bz) ^ shift for bx in range(2) for bz in range(2)]


def near_sums_kernel(
    shifts_in, pos_in, vel_in, thermal_in, offsets_in, occupancy_in,
    pos, thermal, rel, code, geo, wsum, yup, ydn,
    vel, offsets, occupancy, value, ends, shifts, sems, shift_sem,
):
    slots, rows, cols, depth = code.shape
    pairs = [(pos_in, pos), (vel_in, vel), (thermal_in, thermal)]
    flats = [(offsets_in, offsets), (occupancy_in, occupancy)]
    chunks = [(row, tile) for row in range(rows) for tile in range(cols // 8)]
    shift_copy = pltpu.make_async_copy(shifts_in, shifts, shift_sem)
    shift_copy.start()
    copies = []
    for index, (row, tile) in enumerate(chunks):
        at = pl.ds(8 * tile, 8)
        group = []
        for source, target in pairs:
            group.append((source.at[:, :, row, at, :], target.at[:, :, row, at, :]))
        for source, target in flats:
            group.append((source.at[:, row, at, :], target.at[:, row, at, :]))
        copies.append(
            [pltpu.make_async_copy(*ends_, sems.at[index, n]) for n, ends_ in enumerate(group)]
        )
        for copy in copies[-1]:
            copy.start()
    shift_copy.wait()
    for index, (row, tile) in enumerate(chunks):
        at = pl.ds(8 * tile, 8)
        for copy in copies[index]:
            copy.wait()
        groups = four(1 if tile == 0 else 0, shifts[0])
        for lanes in halves(depth):
            for slot in range(slots):
                code[slot, row, at, lanes] = jnp.where(
                    occupancy[slot, row, at, lanes] == 1, offsets[slot, row, at, lanes], GROUPS
                )
                for c in range(3):
                    rel[c, slot, row, at, lanes] = (
                        vel[c, slot, row, at, lanes] - thermal[c, slot, row, at, lanes]
                    )
            chunk_sums(pos, rel, code, value, geo, wsum, groups, row, at, lanes)
    for out, by, col in ((yup, 0, cols - 1), (ydn, 1, 0)):
        for bz in range(2):
            for bx in range(2):
                frame = 4 * bx + 2 * by + bz
                o = frame ^ shifts[0]
                for row in range(rows):
                    own = geo_frame(geo, o, frame, row, pl.ds(col, 1))
                    own.update(vel_frame(wsum, o, frame, row, pl.ds(col, 1)))
                    for v in range(16):
                        if bx == 1 and row == 1:
                            ends[bz, 1, v : v + 1, :] += own[v]
                        else:
                            ends[bz, row + 1 - bx, v : v + 1, :] = own[v]
        for r in range(3):
            out[r] = ends[0, r] + roll(ends[1, r], -1)


def rest_sums_kernel(
    shifts, pos, rel, code, geo_near, wsum_near, geo, wsum, row0, row1, row2, value, part, shifted
):
    _, rows, cols, depth = code.shape
    for row in range(rows):
        for tile in range(cols // 8):
            at = pl.ds(8 * tile, 8)
            far = 0 if tile == 0 else 1
            for o in four(1 - far, shifts[0]):
                for v in range(10):
                    geo[o, v, row, at, :] = geo_near[o, v, row, at, :]
                for v in range(6):
                    wsum[o, v, row, at, :] = wsum_near[o, v, row, at, :]
            groups = four(far, shifts[0])
            for lanes in halves(depth):
                chunk_sums(pos, rel, code, value, geo, wsum, groups, row, at, lanes)
    outs = (row0, row1, row2)
    expand(lambda *where: geo_frame(geo, *where), GEO, shifts[0], outs, None, None, part, shifted)
    expand(lambda *where: vel_frame(wsum, *where), VEL, shifts[0], outs, None, None, part, shifted)


def change_sums_kernel(step, pos, thermal, code, dsum, value):
    slots, rows, cols, depth = code.shape
    tiles = cols // 8

    def chunk(index, carry):
        row = index // tiles
        at = pl.ds(pl.multiple_of(8 * (index % tiles), 8), 8)
        for lanes in halves(depth):
            for slot in range(slots):
                p = [pos[c, slot, row, at, lanes] for c in range(3)]
                d = [
                    thermal[c, (slot + step) % slots, row, at, lanes]
                    - thermal[c, (slot + step + 1) % slots, row, at, lanes]
                    for c in range(3)
                ]
                for name, term in enumerate(d + cross(p, d)):
                    value[name, slot] = term
            codes = [code[slot, row, at, lanes] for slot in range(slots)]
            for base in (0, 4):

                def store(index, g, total):
                    dsum[base + g, index, row, at, lanes] = total

                accumulate(value, codes, range(base, base + 4), list(range(6)), store)
        return carry

    lax.fori_loop(0, rows * tiles, chunk, 0)


def roll(value, amount):
    return pltpu.roll(value, amount % value.shape[-1], value.ndim - 1)


GEO = (0, 1, 2, 3, 10, 11, 12, 13, 14, 15)
VEL = (4, 5, 6, 7, 8, 9)


def geo_frame(geo, o, frame, row, at):
    b = bits(frame)
    n = geo[o, 0, row, at, :]
    s = [geo[o, 1 + c, row, at, :] for c in range(3)]
    q = [s[c] + n if b[c] else s[c] for c in range(3)]
    out = {0: n, 1: q[0], 2: q[1], 3: q[2]}
    for k, (i, j) in enumerate(((0, 0), (1, 1), (2, 2), (0, 1), (0, 2), (1, 2))):
        value = geo[o, 4 + k, row, at, :]
        if b[i]:
            value = value + s[j]
        if b[j]:
            value = value + q[i]
        out[10 + k] = value
    return out


def vel_frame(wsum, o, frame, row, at):
    bx, by, bz = bits(frame)
    w = [wsum[o, c, row, at, :] for c in range(3)]
    l = [wsum[o, 3 + c, row, at, :] for c in range(3)]
    if bx:
        l = [l[0], l[1] - w[2], l[2] + w[1]]
    if by:
        l = [l[0] + w[2], l[1], l[2] - w[0]]
    if bz:
        l = [l[0] - w[1], l[1] + w[0], l[2]]
    return dict(zip(VEL, w + l))


def expand(frame_of, names, shift, rows, yup, ydn, part, shifted):
    cols = rows[0].shape[1]
    every = pl.ds(0, cols)
    for by in range(2):
        for bz in range(2):
            for bx in range(2):
                frame = 4 * bx + 2 * by + bz
                for row in range(2):
                    values = frame_of(frame ^ shift, frame, row, every)
                    for v in names:
                        if bx == 1 and row == 1:
                            part[by, bz, 1, v] += values[v]
                        else:
                            part[by, bz, row + 1 - bx, v] = values[v]
    for r in range(3):
        for v in names:
            near = part[0, 0, r, v] + roll(part[0, 1, r, v], -1)
            beyond = part[1, 0, r, v] + roll(part[1, 1, r, v], -1)
            shifted[r, v, cols:, :] = jnp.zeros((8, beyond.shape[1]), F32)
            shifted[r, v, :cols, :] = beyond
            main = near + shifted[r, v, 1 : cols + 1, :]
            rows[r][v] = main
            rows[r][16, v : v + 1, :] = beyond[0:1]
            if yup is not None:
                yup[r, v : v + 1, :] = main[cols - 1 : cols]
                ydn[r, v : v + 1, :] = beyond[0:1]


def geometry_kernel(step, shifts, geo, row0, row1, row2, yup, ydn, part, shifted):
    outs = (row0, row1, row2)
    expand(
        lambda *where: geo_frame(geo, *where), GEO, shifts[step], outs, yup, ydn, part, shifted
    )


def corner_kernel(yprev, ynext, low, high):
    for out, r in ((low, 0), (high, 2)):
        out[0] = yprev[r]
        out[1] = ynext[r]


def complete_row(row, ends, out):
    last = out.shape[1] - 1
    for v in range(16):
        out[v] = plus([part[v] for part in row])
    out[16] = plus([part[16] for part in row] + [low for low, _ in ends])
    add = plus([high for _, high in ends])
    for v in range(16):
        out[v, last : last + 1, :] += add[v : v + 1]


def solve(sums):
    inverse = 1.0 / jnp.maximum(sums[0], 1.0)
    first = sums[1:4]
    flow = sums[4:7]
    centre = [value * inverse for value in first]
    drift = [value * inverse for value in flow]
    moment = cross(centre, flow)
    torque = [sums[7 + c] - moment[c] for c in range(3)]
    mxx = sums[10] - first[0] * centre[0]
    myy = sums[11] - first[1] * centre[1]
    mzz = sums[12] - first[2] * centre[2]
    kxy = first[0] * centre[1] - sums[13]
    kxz = first[0] * centre[2] - sums[14]
    kyz = first[1] * centre[2] - sums[15]
    kxx = myy + mzz + RIDGE
    kyy = mxx + mzz + RIDGE
    kzz = mxx + myy + RIDGE
    adj_xx = kyy * kzz - kyz * kyz
    adj_yy = kxx * kzz - kxz * kxz
    adj_zz = kxx * kyy - kxy * kxy
    adj_xy = kxz * kyz - kxy * kzz
    adj_xz = kxy * kyz - kxz * kyy
    adj_yz = kxy * kxz - kxx * kyz
    scale = 1.0 / (kxx * adj_xx + kxy * adj_xy + kxz * adj_xz)
    spin = [
        (adj_xx * torque[0] + adj_xy * torque[1] + adj_xz * torque[2]) * scale,
        (adj_xy * torque[0] + adj_yy * torque[1] + adj_yz * torque[2]) * scale,
        (adj_xz * torque[0] + adj_yz * torque[1] + adj_zz * torque[2]) * scale,
    ]
    turned = cross(spin, centre)
    return [drift[c] - turned[c] for c in range(3)] + spin


def fill_table(own, around, table, total):
    yprev, ynext, xprev, xnext, cprev, cnext = around
    cols = own[0].shape[1]
    for r in range(3):
        row, ends = [own[r]], [(yprev[r], ynext[r])]
        if r != 1:
            row.append(xprev if r == 0 else xnext)
            corner = cprev if r == 0 else cnext
            ends.append((corner[0], corner[1]))
        complete_row(row, ends, total)
        for t in range(cols // 8):
            at = pl.ds(8 * t, 8)
            state = solve([total[v, at, :] for v in range(16)])
            for v in range(6):
                table[0, v, r, 8 + 8 * t : 16 + 8 * t, :] = state[v]
                table[1, v, r, 8 + 8 * t : 16 + 8 * t, :] = roll(state[v], 1)
        state = solve([total[16, v : v + 1, :] for v in range(16)])
        for v in range(6):
            wide = jnp.broadcast_to(state[v], (8, state[v].shape[1]))
            table[0, v, r, 0:8, :] = wide
            table[1, v, r, 0:8, :] = roll(wide, 1)


def shift_a(a, spin, b):
    a = list(a)
    if b[0]:
        a = [a[0], a[1] + spin[2], a[2] - spin[1]]
    if b[1]:
        a = [a[0] - spin[2], a[1], a[2] + spin[0]]
    if b[2]:
        a = [a[0] + spin[1], a[1] - spin[0], a[2]]
    return a


def update_groups(geo, dsum, shift, table, wsum):
    cols = geo.shape[3]
    for code in range(GROUPS):
        bx, by, bz = bits(code)
        o = code ^ shift
        for row in range(2):
            for t in range(cols // 8):
                at = pl.ds(8 * t, 8)
                from_col = 8 + 8 * t - by
                values = [table[bz, v, row + 1 - bx, from_col : from_col + 8, :] for v in range(6)]
                spin = values[3:]
                a = shift_a(values[:3], spin, (bx, by, bz))
                n = geo[o, 0, row, at, :]
                s = [geo[o, 1 + c, row, at, :] for c in range(3)]
                xx, yy, zz, xy, xz, yz = [geo[o, 4 + c, row, at, :] for c in range(6)]
                turn = cross(spin, s)
                arm = cross(s, a)
                own = [
                    (yy + zz) * spin[0] - xy * spin[1] - xz * spin[2],
                    (xx + zz) * spin[1] - xy * spin[0] - yz * spin[2],
                    (xx + yy) * spin[2] - xz * spin[0] - yz * spin[1],
                ]
                for c in range(3):
                    wsum[o, c, row, at, :] = dsum[o, c, row, at, :] + n * a[c] + turn[c]
                    wsum[o, 3 + c, row, at, :] = dsum[o, 3 + c, row, at, :] + arm[c] + own[c]


def step_kernel(
    step, shifts, geo, dsum, own0, own1, own2, yprev, ynext, xprev, xnext, cprev, cnext,
    geo0, geo1, geo2, geoup, geodn,
    row0, row1, row2, yup, ydn, total, table, wsum, part, shifted,
):
    fill_table((own0, own1, own2), (yprev, ynext, xprev, xnext, cprev, cnext), table, total)
    update_groups(geo, dsum, shifts[step], table, wsum)
    rows = (row0, row1, row2)
    for target, source in zip(rows, (geo0, geo1, geo2)):
        for v in GEO:
            target[v] = source[v]
        target[16] = source[16]
    yup[...] = geoup[...]
    ydn[...] = geodn[...]
    expand(lambda *where: vel_frame(wsum, *where), VEL, shifts[step + 1], rows, yup, ydn, part, shifted)


def last_kernel(own0, own1, own2, yprev, ynext, xprev, xnext, cprev, cnext, table, total):
    fill_table((own0, own1, own2), (yprev, ynext, xprev, xnext, cprev, cnext), table, total)


def particles_kernel(shifts, table, pos, thermal, code, out, variants):
    slots = code.shape[0]
    row = pl.program_id(0)
    tile = pl.program_id(1)
    for half in range(pos.shape[4] // 128):
        lanes = pl.ds(half * 128, 128)
        for frame in range(GROUPS):
            bx, by, bz = bits(frame)
            values = [
                table[bz, v, row + 1 - bx, pl.ds(8 * tile, 16), lanes][8 - by : 16 - by]
                for v in range(6)
            ]
            values[:3] = shift_a(values[:3], values[3:], (bx, by, bz))
            for v in range(6):
                variants[frame, v] = values[v]
        for slot in range(slots):
            base = code[slot, 0, :, lanes]
            k = base ^ shifts[STEPS - 1]
            isx, isy, isz = (k & 4) != 0, (k & 2) != 0, (k & 1) != 0
            used = base < GROUPS
            state = []
            for v in range(6):
                level = [jnp.where(isx, variants[4 + i, v], variants[i, v]) for i in range(4)]
                level = [jnp.where(isy, level[2 + i], level[i]) for i in range(2)]
                state.append(jnp.where(isz, level[1], level[0]))
            p = [pos[c, slot, 0, :, lanes] for c in range(3)]
            turn = cross(state[3:], p)
            for c in range(3):
                fresh = thermal[c, (slot + STEPS - 1) % slots, 0, :, lanes] + (state[c] + turn[c])
                out[c, slot, 0, :, lanes] = jnp.where(used, fresh, 0.0)


VMEM = pl.BlockSpec(memory_space=pltpu.VMEM)
SMEM = pl.BlockSpec(memory_space=pltpu.SMEM)
HBM = pl.BlockSpec(memory_space=pltpu.HBM)


def in_hbm(value):
    return pltpu.with_memory_space_constraint(value, pltpu.HBM)


def params(mib):
    return pltpu.CompilerParams(vmem_limit_bytes=mib * 2**20)


def shape(*dims):
    return jax.ShapeDtypeStruct(dims, F32)


def big_spec(lead):
    return pl.BlockSpec((*lead, 1, 8, 256), lambda r, t: (*([0] * len(lead)), r, t, 0))


def local(positions, velocities, thermal, offsets, occupancy, shift_codes):
    slots, rows, cols, depth = offsets.shape
    grid = (rows, cols // 8)
    vec = big_spec((3, slots))
    flat = big_spec((slots,))
    group = lambda count: pltpu.VMEM((GROUPS, count, rows, cols, depth), F32)
    group_shape = lambda count: shape(GROUPS, count, rows, cols, depth)
    value = lambda count: pltpu.VMEM((count, slots, 8, 128), F32)
    vec_shape = shape(3, slots, rows, cols, depth)
    flat_shape = jax.ShapeDtypeStruct((slots, rows, cols, depth), jnp.int32)
    row_shape = shape(17, cols, depth)
    col_shape = shape(3, 16, depth)
    expand_out = [row_shape] * 3 + [col_shape] * 2
    expand_scratch = [
        pltpu.VMEM((2, 2, 3, 16, cols, depth), F32),
        pltpu.VMEM((3, 16, cols + 8, depth), F32),
    ]
    total = pltpu.VMEM((17, cols, depth), F32)
    table_shape = (2, 6, 3, cols + 8, depth)

    pos, hot, rel, code, geo_near, wsum_near, yup, ydn = pl.pallas_call(
        near_sums_kernel,
        in_specs=[HBM] * 6,
        out_specs=[VMEM] * 8,
        out_shape=[vec_shape] * 3 + [flat_shape, group_shape(10), group_shape(6)] + [col_shape] * 2,
        scratch_shapes=[
            pltpu.VMEM(vec_shape.shape, F32),
            pltpu.VMEM(flat_shape.shape, jnp.int32),
            pltpu.VMEM(flat_shape.shape, jnp.int32),
            value(15),
            pltpu.VMEM((2, 3, 16, depth), F32),
            pltpu.SMEM((STEPS,), jnp.int32),
            pltpu.SemaphoreType.DMA((rows * cols // 8, 5)),
            pltpu.SemaphoreType.DMA,
        ],
        compiler_params=params(16),
        name="near_sums",
    )(*map(in_hbm, (shift_codes, positions, velocities, thermal, offsets, occupancy)))

    def ring(axis, by):
        count = lax.axis_size(axis)
        return [(i, (i + by) % count) for i in range(count)]

    def change_sums(step):
        return pl.pallas_call(
            functools.partial(change_sums_kernel, step),
            in_specs=[VMEM] * 3,
            out_specs=VMEM,
            out_shape=group_shape(6),
            scratch_shapes=[value(6)],
            compiler_params=params(8),
            name="change_sums",
        )(pos, hot, code)

    def geometry(step):
        return pl.pallas_call(
            functools.partial(geometry_kernel, step),
            in_specs=[SMEM, VMEM],
            out_specs=[VMEM] * 5,
            out_shape=expand_out,
            scratch_shapes=expand_scratch,
            compiler_params=params(12),
            name="geometry",
        )(shift_codes, geo)

    def send(value, axis, by):
        return lax.ppermute(value, axis, ring(axis, by))

    for step in range(STEPS):
        yprev = send(yup, "gy", 1)
        ynext = send(ydn, "gy", -1)
        if step == 0:
            geo, _, row0, row1, row2 = pl.pallas_call(
                rest_sums_kernel,
                in_specs=[SMEM] + [VMEM] * 5,
                out_specs=[VMEM] * 5,
                out_shape=[group_shape(10), group_shape(6)] + [row_shape] * 3,
                scratch_shapes=[value(15)] + expand_scratch,
                compiler_params=params(16),
                name="rest_sums",
            )(shift_codes, pos, rel, code, geo_near, wsum_near)
        xprev = send(row2, "gx", 1)
        xnext = send(row0, "gx", -1)
        low, high = pl.pallas_call(
            corner_kernel,
            in_specs=[VMEM] * 2,
            out_specs=[VMEM] * 2,
            out_shape=[shape(2, 16, depth)] * 2,
            compiler_params=params(2),
            name="corners",
        )(yprev, ynext)
        cprev = send(high, "gx", 1)
        cnext = send(low, "gx", -1)
        found = (row0, row1, row2, yprev, ynext, xprev, xnext, cprev, cnext)
        if step + 1 < STEPS:
            dsum = change_sums(step)
            ahead = geometry(step + 1)
            row0, row1, row2, yup, ydn = pl.pallas_call(
                functools.partial(step_kernel, step),
                in_specs=[SMEM] + [VMEM] * 16,
                out_specs=[VMEM] * 5,
                out_shape=expand_out,
                scratch_shapes=[total, pltpu.VMEM(table_shape, F32), group(6)] + expand_scratch,
                compiler_params=params(16),
                name="step",
            )(shift_codes, geo, dsum, *found, *ahead)

    table = pl.pallas_call(
        last_kernel,
        in_specs=[VMEM] * 9,
        out_specs=VMEM,
        out_shape=shape(*table_shape),
        scratch_shapes=[total],
        compiler_params=params(6),
        name="last",
    )(*found)

    return pl.pallas_call(
        particles_kernel,
        grid=grid,
        in_specs=[SMEM, VMEM, vec, vec, flat],
        out_specs=vec,
        out_shape=vec_shape,
        scratch_shapes=[pltpu.VMEM((GROUPS, 6, 8, 128), F32)],
        compiler_params=params(12),
        name="particles",
    )(shift_codes, table, pos, hot, code)


def solution(mesh):
    in_specs = (
        P(None, None, "gx", "gy", None),
        P(None, None, "gx", "gy", None),
        P(None, None, "gx", "gy", None),
        P(None, "gx", "gy", None),
        P(None, "gx", "gy", None),
        P(),
    )
    out_specs = P(None, None, "gx", "gy", None)
    return jax.shard_map(local, mesh=mesh, in_specs=in_specs, out_specs=out_specs, check_vma=False)
```

```python
import functools

import jax
import jax.numpy as jnp
from jax import lax
from jax.experimental import pallas as pl
from jax.experimental.pallas import tpu as pltpu
from jax.sharding import PartitionSpec as P


STEPS = 3
RIDGE = 0.5
GROUPS = 8
F32 = jnp.float32


def bits(code):
    return code // 4, code // 2 % 2, code % 2


def is_even(axis):
    return lax.axis_index(axis) % 2 == 0


def cross(u, v):
    return [
        u[1] * v[2] - u[2] * v[1],
        u[2] * v[0] - u[0] * v[2],
        u[0] * v[1] - u[1] * v[0],
    ]


def accumulate(value_ref, codes, groups, names, store):
    sums = [[None] * len(groups) for _ in names]
    for slot, code in enumerate(codes):
        masks = [code == group for group in groups]
        for at, name in enumerate(names):
            value = 1.0 if name is None else value_ref[name, slot]
            for g, mask in enumerate(masks):
                part = jnp.where(mask, value, 0.0)
                old = sums[at][g]
                sums[at][g] = part if old is None else old + part
    for at in range(len(names)):
        for g in range(len(groups)):
            store(at, g, sums[at][g])


def moments(p, w):
    seconds = [p[0] * p[0], p[1] * p[1], p[2] * p[2], p[0] * p[1], p[0] * p[2], p[1] * p[2]]
    return p + seconds + w + cross(p, w)


def chunk_sums(pos, rel, code, value, geo, wsum, groups, row, at, lanes):
    slots = code.shape[0]
    for slot in range(slots):
        p = [pos[c, slot, row, at, lanes] for c in range(3)]
        w = [rel[c, slot, row, at, lanes] for c in range(3)]
        for name, term in enumerate(moments(p, w)):
            value[name, slot] = term
    codes = [code[slot, row, at, lanes] for slot in range(slots)]

    def store_first(index, g, total):
        geo[groups[g], index, row, at, lanes] = total

    def store_second(index, g, total):
        if index < 2:
            geo[groups[g], 8 + index, row, at, lanes] = total
        else:
            wsum[groups[g], index - 2, row, at, lanes] = total

    accumulate(value, codes, groups, [None] + list(range(7)), store_first)
    accumulate(value, codes, groups, list(range(7, 15)), store_second)


def halves(depth):
    return [pl.ds(128 * half, 128) for half in range(depth // 128)]


def four(by, shift):
    return [(4 * bx + 2 * by + bz) ^ shift for bx in range(2) for bz in range(2)]


def near_sums_kernel(
    shifts_in, pos_in, vel_in, thermal_in, offsets_in, occupancy_in,
    pos, thermal, rel, code, geo, wsum, y_in, y_out,
    vel, offsets, occupancy, value, ends, shifts, sems, shift_sem,
):
    slots, rows, cols, depth = code.shape
    pairs = [(pos_in, pos), (vel_in, vel), (thermal_in, thermal)]
    flats = [(offsets_in, offsets), (occupancy_in, occupancy)]
    chunks = [(row, tile) for row in range(rows) for tile in range(cols // 8)]
    shift_copy = pltpu.make_async_copy(shifts_in, shifts, shift_sem)
    shift_copy.start()
    copies = []
    for index, (row, tile) in enumerate(chunks):
        at = pl.ds(8 * tile, 8)
        group = []
        for source, target in pairs:
            group.append((source.at[:, :, row, at, :], target.at[:, :, row, at, :]))
        for source, target in flats:
            group.append((source.at[:, row, at, :], target.at[:, row, at, :]))
        copies.append(
            [pltpu.make_async_copy(*ends_, sems.at[index, n]) for n, ends_ in enumerate(group)]
        )
        for copy in copies[-1]:
            copy.start()
    shift_copy.wait()
    for index, (row, tile) in enumerate(chunks):
        at = pl.ds(8 * tile, 8)
        for copy in copies[index]:
            copy.wait()
        groups = four(1 if tile == 0 else 0, shifts[0])
        for lanes in halves(depth):
            for slot in range(slots):
                code[slot, row, at, lanes] = jnp.where(
                    occupancy[slot, row, at, lanes] == 1, offsets[slot, row, at, lanes], GROUPS
                )
                for c in range(3):
                    rel[c, slot, row, at, lanes] = (
                        vel[c, slot, row, at, lanes] - thermal[c, slot, row, at, lanes]
                    )
            chunk_sums(pos, rel, code, value, geo, wsum, groups, row, at, lanes)

    def frame_of(*where):
        return {**geo_frame(geo, *where), **vel_frame(wsum, *where)}

    up, down = edges(frame_of, range(16), shifts[0], ends, cols)
    even = is_even("gy")
    for r in range(3):
        y_in[r] = jnp.where(even, up[r], down[r])
        y_out[r] = jnp.where(even, down[r], up[r])


def rest_sums_kernel(
    shifts, pos, rel, code, geo_near, wsum_near,
    geo, wsum, far, mid, near, value, low, high, part, shifted,
):
    _, rows, cols, depth = code.shape
    for row in range(rows):
        for tile in range(cols // 8):
            at = pl.ds(8 * tile, 8)
            by = 0 if tile == 0 else 1
            for o in four(1 - by, shifts[0]):
                for v in range(10):
                    geo[o, v, row, at, :] = geo_near[o, v, row, at, :]
                for v in range(6):
                    wsum[o, v, row, at, :] = wsum_near[o, v, row, at, :]
            groups = four(by, shifts[0])
            for lanes in halves(depth):
                chunk_sums(pos, rel, code, value, geo, wsum, groups, row, at, lanes)
    outs = (low, mid, high)
    expand(lambda *where: geo_frame(geo, *where), GEO, shifts[0], outs, None, None, part, shifted)
    expand(lambda *where: vel_frame(wsum, *where), VEL, shifts[0], outs, None, None, part, shifted)
    by_role(is_even("gx"), low, high, far, near)


def change_sums_kernel(step, pos, thermal, code, dsum, value):
    slots, rows, cols, depth = code.shape
    tiles = cols // 8

    def chunk(index, carry):
        row = index // tiles
        at = pl.ds(pl.multiple_of(8 * (index % tiles), 8), 8)
        for lanes in halves(depth):
            for slot in range(slots):
                p = [pos[c, slot, row, at, lanes] for c in range(3)]
                d = [
                    thermal[c, (slot + step) % slots, row, at, lanes]
                    - thermal[c, (slot + step + 1) % slots, row, at, lanes]
                    for c in range(3)
                ]
                for name, term in enumerate(d + cross(p, d)):
                    value[name, slot] = term
            codes = [code[slot, row, at, lanes] for slot in range(slots)]
            for base in (0, 4):

                def store(index, g, total):
                    dsum[base + g, index, row, at, lanes] = total

                accumulate(value, codes, range(base, base + 4), list(range(6)), store)
        return carry

    lax.fori_loop(0, rows * tiles, chunk, 0)


def roll(value, amount):
    return pltpu.roll(value, amount % value.shape[-1], value.ndim - 1)


GEO = (0, 1, 2, 3, 10, 11, 12, 13, 14, 15)
VEL = (4, 5, 6, 7, 8, 9)


def geo_frame(geo, o, frame, row, at):
    b = bits(frame)
    n = geo[o, 0, row, at, :]
    s = [geo[o, 1 + c, row, at, :] for c in range(3)]
    q = [s[c] + n if b[c] else s[c] for c in range(3)]
    out = {0: n, 1: q[0], 2: q[1], 3: q[2]}
    for k, (i, j) in enumerate(((0, 0), (1, 1), (2, 2), (0, 1), (0, 2), (1, 2))):
        value = geo[o, 4 + k, row, at, :]
        if b[i]:
            value = value + s[j]
        if b[j]:
            value = value + q[i]
        out[10 + k] = value
    return out


def vel_frame(wsum, o, frame, row, at):
    bx, by, bz = bits(frame)
    w = [wsum[o, c, row, at, :] for c in range(3)]
    l = [wsum[o, 3 + c, row, at, :] for c in range(3)]
    if bx:
        l = [l[0], l[1] - w[2], l[2] + w[1]]
    if by:
        l = [l[0] + w[2], l[1], l[2] - w[0]]
    if bz:
        l = [l[0] - w[1], l[1] + w[0], l[2]]
    return dict(zip(VEL, w + l))


def expand(frame_of, names, shift, rows, yup, ydn, part, shifted):
    cols = rows[0].shape[1]
    every = pl.ds(0, cols)
    for by in range(2):
        for bz in range(2):
            for bx in range(2):
                frame = 4 * bx + 2 * by + bz
                for row in range(2):
                    values = frame_of(frame ^ shift, frame, row, every)
                    for v in names:
                        if bx == 1 and row == 1:
                            part[by, bz, 1, v] += values[v]
                        else:
                            part[by, bz, row + 1 - bx, v] = values[v]
    for r in range(3):
        for v in names:
            near = part[0, 0, r, v] + roll(part[0, 1, r, v], -1)
            beyond = part[1, 0, r, v] + roll(part[1, 1, r, v], -1)
            shifted[r, v, cols:, :] = jnp.zeros((8, beyond.shape[1]), F32)
            shifted[r, v, :cols, :] = beyond
            main = near + shifted[r, v, 1 : cols + 1, :]
            rows[r][v] = main
            rows[r][16, v : v + 1, :] = beyond[0:1]
            if yup is not None:
                yup[r, v : v + 1, :] = main[cols - 1 : cols]
                ydn[r, v : v + 1, :] = beyond[0:1]


def edges(frame_of, names, shift, ends, cols):
    found = []
    for by, col in ((0, cols - 1), (1, 0)):
        for bz in range(2):
            for bx in range(2):
                frame = 4 * bx + 2 * by + bz
                for row in range(2):
                    own = frame_of(frame ^ shift, frame, row, pl.ds(col, 1))
                    for v in names:
                        if bx == 1 and row == 1:
                            ends[bz, 1, v : v + 1, :] += own[v]
                        else:
                            ends[bz, row + 1 - bx, v : v + 1, :] = own[v]
        found.append([ends[0, r] + roll(ends[1, r], -1) for r in range(3)])
    return found


def geometry_kernel(step, shifts, geo, row0, row1, row2, yup, ydn, part, shifted):
    outs = (row0, row1, row2)
    yup[...] = jnp.zeros_like(yup)
    ydn[...] = jnp.zeros_like(ydn)
    expand(
        lambda *where: geo_frame(geo, *where), GEO, shifts[step], outs, yup, ydn, part, shifted
    )


def by_role(even, first, second, one, two):
    for at in range(first.shape[0]):
        one[at] = jnp.where(even, first[at], second[at])
        two[at] = jnp.where(even, second[at], first[at])


def y_parts(y_in, y_out, r):
    even = is_even("gy")
    return jnp.where(even, y_out[r], y_in[r]), jnp.where(even, y_in[r], y_out[r])


def complete_row(row, low, high, out):
    last = out.shape[1] - 1
    out[...] = row[...]
    out[16] = row[16] + low
    for v in range(16):
        out[v, last : last + 1, :] = row[v, last : last + 1, :] + high[v : v + 1]


def fold_kernel(far, near, y_in, y_out, far_out, near_out):
    even = is_even("gx")
    low, high = y_parts(y_in, y_out, 0), y_parts(y_in, y_out, 2)
    far_ends = [jnp.where(even, low[at], high[at]) for at in range(2)]
    near_ends = [jnp.where(even, high[at], low[at]) for at in range(2)]
    complete_row(far, *far_ends, far_out)
    complete_row(near, *near_ends, near_out)


def solve(sums):
    inverse = 1.0 / jnp.maximum(sums[0], 1.0)
    first = sums[1:4]
    flow = sums[4:7]
    centre = [value * inverse for value in first]
    drift = [value * inverse for value in flow]
    moment = cross(centre, flow)
    torque = [sums[7 + c] - moment[c] for c in range(3)]
    mxx = sums[10] - first[0] * centre[0]
    myy = sums[11] - first[1] * centre[1]
    mzz = sums[12] - first[2] * centre[2]
    kxy = first[0] * centre[1] - sums[13]
    kxz = first[0] * centre[2] - sums[14]
    kyz = first[1] * centre[2] - sums[15]
    kxx = myy + mzz + RIDGE
    kyy = mxx + mzz + RIDGE
    kzz = mxx + myy + RIDGE
    adj_xx = kyy * kzz - kyz * kyz
    adj_yy = kxx * kzz - kxz * kxz
    adj_zz = kxx * kyy - kxy * kxy
    adj_xy = kxz * kyz - kxy * kzz
    adj_xz = kxy * kyz - kxz * kyy
    adj_yz = kxy * kxz - kxx * kyz
    scale = 1.0 / (kxx * adj_xx + kxy * adj_xy + kxz * adj_xz)
    spin = [
        (adj_xx * torque[0] + adj_xy * torque[1] + adj_xz * torque[2]) * scale,
        (adj_xy * torque[0] + adj_yy * torque[1] + adj_yz * torque[2]) * scale,
        (adj_xz * torque[0] + adj_yz * torque[1] + adj_zz * torque[2]) * scale,
    ]
    turned = cross(spin, centre)
    return [drift[c] - turned[c] for c in range(3)] + spin


def fill_table(own, around, table, total):
    far, mid, near = own
    y_in, y_out, x_far, x_near = around
    cols = mid.shape[1]
    even = is_even("gx")
    complete_row(mid, *y_parts(y_in, y_out, 1), total)
    for r in range(3):
        if r == 1:
            read = lambda v, at: total[v, at, :]
        else:
            mine = even if r == 0 else jnp.logical_not(even)
            read = lambda v, at: jnp.where(
                mine, far[v, at, :] + x_far[v, at, :], near[v, at, :] + x_near[v, at, :]
            )
        for t in range(cols // 8):
            at = pl.ds(8 * t, 8)
            state = solve([read(v, at) for v in range(16)])
            for v in range(6):
                table[0, v, r, 8 + 8 * t : 16 + 8 * t, :] = state[v]
                table[1, v, r, 8 + 8 * t : 16 + 8 * t, :] = roll(state[v], 1)
        state = solve([read(16, pl.ds(v, 1)) for v in range(16)])
        for v in range(6):
            wide = jnp.broadcast_to(state[v], (8, state[v].shape[1]))
            table[0, v, r, 0:8, :] = wide
            table[1, v, r, 0:8, :] = roll(wide, 1)


def shift_a(a, spin, b):
    a = list(a)
    if b[0]:
        a = [a[0], a[1] + spin[2], a[2] - spin[1]]
    if b[1]:
        a = [a[0] - spin[2], a[1], a[2] + spin[0]]
    if b[2]:
        a = [a[0] + spin[1], a[1] - spin[0], a[2]]
    return a


def update_groups(geo, dsum, shift, table, wsum):
    cols = geo.shape[3]
    for code in range(GROUPS):
        bx, by, bz = bits(code)
        o = code ^ shift
        for row in range(2):
            for t in range(cols // 8):
                at = pl.ds(8 * t, 8)
                from_col = 8 + 8 * t - by
                values = [table[bz, v, row + 1 - bx, from_col : from_col + 8, :] for v in range(6)]
                spin = values[3:]
                a = shift_a(values[:3], spin, (bx, by, bz))
                n = geo[o, 0, row, at, :]
                s = [geo[o, 1 + c, row, at, :] for c in range(3)]
                xx, yy, zz, xy, xz, yz = [geo[o, 4 + c, row, at, :] for c in range(6)]
                turn = cross(spin, s)
                arm = cross(s, a)
                own = [
                    (yy + zz) * spin[0] - xy * spin[1] - xz * spin[2],
                    (xx + zz) * spin[1] - xy * spin[0] - yz * spin[2],
                    (xx + yy) * spin[2] - xz * spin[0] - yz * spin[1],
                ]
                for c in range(3):
                    wsum[o, c, row, at, :] = dsum[o, c, row, at, :] + n * a[c] + turn[c]
                    wsum[o, 3 + c, row, at, :] = dsum[o, 3 + c, row, at, :] + arm[c] + own[c]


def step_kernel(
    step, shifts, geo, dsum, far, mid, near, y_in, y_out, x_far, x_near, geoup, geodn,
    wsum, next_in, next_out, total, table, ends,
):
    cols = mid.shape[1]
    fill_table((far, mid, near), (y_in, y_out, x_far, x_near), table, total)
    update_groups(geo, dsum, shifts[step], table, wsum)
    for bz in range(2):
        for r in range(3):
            ends[bz, r] = jnp.zeros_like(ends[bz, r])
    up, down = edges(
        lambda *where: vel_frame(wsum, *where), VEL, shifts[step + 1], ends, cols
    )
    even = is_even("gy")
    for r in range(3):
        up_r, down_r = geoup[r] + up[r], geodn[r] + down[r]
        next_in[r] = jnp.where(even, up_r, down_r)
        next_out[r] = jnp.where(even, down_r, up_r)


def rows_kernel(
    step, shifts, wsum, geo0, geo1, geo2, far, mid, near, low, high, part, shifted
):
    rows = (low, mid, high)
    for target, source in zip(rows, (geo0, geo1, geo2)):
        for v in GEO:
            target[v] = source[v]
        target[16] = source[16]
    expand(
        lambda *where: vel_frame(wsum, *where), VEL, shifts[step + 1], rows, None, None, part, shifted
    )
    by_role(is_even("gx"), low, high, far, near)


def particles_kernel(
    shifts, far, mid, near, y_in, y_out, x_far, x_near, pos, thermal, code,
    out, total, table, variants, fresh, sems,
):
    slots, rows, cols, depth = code.shape
    fill_table((far, mid, near), (y_in, y_out, x_far, x_near), table, total)
    copies = []
    for row in range(rows):
        for tile in range(cols // 8):
            at = pl.ds(8 * tile, 8)
            for lanes in halves(depth):
                for frame in range(GROUPS):
                    bx, by, bz = bits(frame)
                    first = 8 + 8 * tile - by
                    values = [
                        table[bz, v, row + 1 - bx, first : first + 8, lanes] for v in range(6)
                    ]
                    values[:3] = shift_a(values[:3], values[3:], (bx, by, bz))
                    for v in range(6):
                        variants[frame, v] = values[v]
                for slot in range(slots):
                    base = code[slot, row, at, lanes]
                    k = base ^ shifts[STEPS - 1]
                    isx, isy, isz = (k & 4) != 0, (k & 2) != 0, (k & 1) != 0
                    used = base < GROUPS
                    state = []
                    for v in range(6):
                        level = [jnp.where(isx, variants[4 + i, v], variants[i, v]) for i in range(4)]
                        level = [jnp.where(isy, level[2 + i], level[i]) for i in range(2)]
                        state.append(jnp.where(isz, level[1], level[0]))
                    turn = cross(state[3:], [pos[c, slot, row, at, lanes] for c in range(3)])
                    for c in range(3):
                        hot = thermal[c, (slot + STEPS - 1) % slots, row, at, lanes]
                        new = hot + (state[c] + turn[c])
                        fresh[c, slot, row, at, lanes] = jnp.where(used, new, 0.0)
            index = len(copies)
            copy = pltpu.make_async_copy(
                fresh.at[:, :, row, at, :], out.at[:, :, row, at, :], sems.at[index]
            )
            copy.start()
            copies.append(copy)
    for copy in copies:
        copy.wait()


VMEM = pl.BlockSpec(memory_space=pltpu.VMEM)
SMEM = pl.BlockSpec(memory_space=pltpu.SMEM)
HBM = pl.BlockSpec(memory_space=pltpu.HBM)


def in_hbm(value):
    return pltpu.with_memory_space_constraint(value, pltpu.HBM)


def params(mib):
    return pltpu.CompilerParams(vmem_limit_bytes=mib * 2**20)


def shape(*dims):
    return jax.ShapeDtypeStruct(dims, F32)


def local(positions, velocities, thermal, offsets, occupancy, shift_codes):
    slots, rows, cols, depth = offsets.shape
    group_shape = lambda count: shape(GROUPS, count, rows, cols, depth)
    value = lambda count: pltpu.VMEM((count, slots, 8, 128), F32)
    vec_shape = shape(3, slots, rows, cols, depth)
    flat_shape = jax.ShapeDtypeStruct((slots, rows, cols, depth), jnp.int32)
    row_shape = shape(17, cols, depth)
    col_shape = shape(3, 16, depth)
    expand_out = [row_shape] * 3 + [col_shape] * 2
    expand_scratch = [
        pltpu.VMEM((2, 2, 3, 16, cols, depth), F32),
        pltpu.VMEM((3, 16, cols + 8, depth), F32),
    ]
    total = pltpu.VMEM((17, cols, depth), F32)
    table_shape = (2, 6, 3, cols + 8, depth)

    pos, hot, rel, code, geo_near, wsum_near, y_in, y_out = pl.pallas_call(
        near_sums_kernel,
        in_specs=[HBM] * 6,
        out_specs=[VMEM] * 8,
        out_shape=[vec_shape] * 3 + [flat_shape, group_shape(10), group_shape(6)] + [col_shape] * 2,
        scratch_shapes=[
            pltpu.VMEM(vec_shape.shape, F32),
            pltpu.VMEM(flat_shape.shape, jnp.int32),
            pltpu.VMEM(flat_shape.shape, jnp.int32),
            value(15),
            pltpu.VMEM((2, 3, 16, depth), F32),
            pltpu.SMEM((STEPS,), jnp.int32),
            pltpu.SemaphoreType.DMA((rows * cols // 8, 5)),
            pltpu.SemaphoreType.DMA,
        ],
        compiler_params=params(16),
        name="near_sums",
    )(*map(in_hbm, (shift_codes, positions, velocities, thermal, offsets, occupancy)))

    def swap(value, axis, odd):
        count = lax.axis_size(axis)
        partner = [(((i + odd) ^ 1) - odd) % count for i in range(count)]
        return lax.ppermute(value, axis, list(enumerate(partner)))

    def change_sums(step):
        return pl.pallas_call(
            functools.partial(change_sums_kernel, step),
            in_specs=[VMEM] * 3,
            out_specs=VMEM,
            out_shape=group_shape(6),
            scratch_shapes=[value(6)],
            compiler_params=params(8),
            name="change_sums",
        )(pos, hot, code)

    def geometry(step):
        return pl.pallas_call(
            functools.partial(geometry_kernel, step),
            in_specs=[SMEM, VMEM],
            out_specs=[VMEM] * 5,
            out_shape=expand_out,
            scratch_shapes=expand_scratch,
            compiler_params=params(12),
            name="geometry",
        )(shift_codes, geo)

    row_scratch = pltpu.VMEM(row_shape.shape, F32)

    for step in range(STEPS):
        got_out = swap(y_out, "gy", 1)
        got_in = swap(y_in, "gy", 0)
        if step == 0:
            geo, wsum, far, mid, near = pl.pallas_call(
                rest_sums_kernel,
                in_specs=[SMEM] + [VMEM] * 5,
                out_specs=[VMEM] * 5,
                out_shape=[group_shape(10), group_shape(6)] + [row_shape] * 3,
                scratch_shapes=[value(15), row_scratch, row_scratch] + expand_scratch,
                compiler_params=params(16),
                name="rest_sums",
            )(shift_codes, pos, rel, code, geo_near, wsum_near)
        else:
            far, mid, near = pl.pallas_call(
                functools.partial(rows_kernel, step - 1),
                in_specs=[SMEM] + [VMEM] * 4,
                out_specs=[VMEM] * 3,
                out_shape=[row_shape] * 3,
                scratch_shapes=[row_scratch, row_scratch] + expand_scratch,
                compiler_params=params(12),
                name="rows",
            )(shift_codes, wsum, *ahead)
        far, near = pl.pallas_call(
            fold_kernel,
            in_specs=[VMEM] * 4,
            out_specs=[VMEM] * 2,
            out_shape=[row_shape] * 2,
            compiler_params=params(2),
            name="fold",
        )(far, near, got_in, got_out)
        x_far = swap(far, "gx", 1)
        x_near = swap(near, "gx", 0)
        found = (far, mid, near, got_in, got_out, x_far, x_near)
        if step + 1 < STEPS:
            dsum = change_sums(step)
            *ahead, geoup, geodn = geometry(step + 1)
            wsum, y_in, y_out = pl.pallas_call(
                functools.partial(step_kernel, step),
                in_specs=[SMEM] + [VMEM] * 11,
                out_specs=[VMEM] * 3,
                out_shape=[group_shape(6)] + [col_shape] * 2,
                scratch_shapes=[
                    total, pltpu.VMEM(table_shape, F32), pltpu.VMEM((2, 3, 16, depth), F32)
                ],
                compiler_params=params(12),
                name="step",
            )(shift_codes, geo, dsum, *found, geoup, geodn)

    sem_count = rows * cols // 8
    return pl.pallas_call(
        particles_kernel,
        in_specs=[SMEM] + [VMEM] * 10,
        out_specs=HBM,
        out_shape=vec_shape,
        scratch_shapes=[
            total, pltpu.VMEM(table_shape, F32), pltpu.VMEM((GROUPS, 6, 8, 128), F32),
            pltpu.VMEM(vec_shape.shape, F32), pltpu.SemaphoreType.DMA((sem_count,)),
        ],
        compiler_params=params(12),
        name="particles",
    )(shift_codes, *found, pos, hot, code)


def solution(mesh):
    in_specs = (
        P(None, None, "gx", "gy", None),
        P(None, None, "gx", "gy", None),
        P(None, None, "gx", "gy", None),
        P(None, "gx", "gy", None),
        P(None, "gx", "gy", None),
        P(),
    )
    out_specs = P(None, None, "gx", "gy", None)
    return jax.shard_map(local, mesh=mesh, in_specs=in_specs, out_specs=out_specs, check_vma=False)
```

```python
import functools

import jax
import jax.numpy as jnp
from jax import lax
from jax.experimental import pallas as pl
from jax.experimental.pallas import tpu as pltpu
from jax.sharding import PartitionSpec as P


STEPS = 3
RIDGE = 0.5
GROUPS = 8
F32 = jnp.float32


def bits(code):
    return code // 4, code // 2 % 2, code % 2


def is_even(axis):
    return lax.axis_index(axis) % 2 == 0


def cross(u, v):
    return [
        u[1] * v[2] - u[2] * v[1],
        u[2] * v[0] - u[0] * v[2],
        u[0] * v[1] - u[1] * v[0],
    ]


def accumulate(value_ref, codes, groups, names, store):
    sums = [[None] * len(groups) for _ in names]
    for slot, code in enumerate(codes):
        masks = [code == group for group in groups]
        for at, name in enumerate(names):
            value = 1.0 if name is None else value_ref[name, slot]
            for g, mask in enumerate(masks):
                part = jnp.where(mask, value, 0.0)
                old = sums[at][g]
                sums[at][g] = part if old is None else old + part
    for at in range(len(names)):
        for g in range(len(groups)):
            store(at, g, sums[at][g])


def moments(p, w):
    seconds = [p[0] * p[0], p[1] * p[1], p[2] * p[2], p[0] * p[1], p[0] * p[2], p[1] * p[2]]
    return p + seconds + w + cross(p, w)


def chunk_sums(pos, rel, code, value, geo, wsum, groups, row, at, lanes):
    slots = code.shape[0]
    for slot in range(slots):
        p = [pos[c, slot, row, at, lanes] for c in range(3)]
        w = [rel[c, slot, row, at, lanes] for c in range(3)]
        for name, term in enumerate(moments(p, w)):
            value[name, slot] = term
    codes = [code[slot, row, at, lanes] for slot in range(slots)]

    def store_first(index, g, total):
        geo[groups[g], index, row, at, lanes] = total

    def store_second(index, g, total):
        if index < 2:
            geo[groups[g], 8 + index, row, at, lanes] = total
        else:
            wsum[groups[g], index - 2, row, at, lanes] = total

    accumulate(value, codes, groups, [None] + list(range(7)), store_first)
    accumulate(value, codes, groups, list(range(7, 15)), store_second)


def halves(depth):
    return [pl.ds(128 * half, 128) for half in range(depth // 128)]


def four(by, shift):
    return [(4 * bx + 2 * by + bz) ^ shift for bx in range(2) for bz in range(2)]


def near_sums_kernel(
    shifts_in, pos_in, vel_in, thermal_in, offsets_in, occupancy_in,
    pos, thermal, rel, code, geo, wsum, y_in, y_out,
    vel, offsets, occupancy, value, ends, shifts, sems, shift_sem,
):
    slots, rows, cols, depth = code.shape
    pairs = [(pos_in, pos), (vel_in, vel), (thermal_in, thermal)]
    flats = [(offsets_in, offsets), (occupancy_in, occupancy)]
    chunks = [(row, tile) for row in range(rows) for tile in range(cols // 8)]
    shift_copy = pltpu.make_async_copy(shifts_in, shifts, shift_sem)
    shift_copy.start()
    copies = []
    for index, (row, tile) in enumerate(chunks):
        at = pl.ds(8 * tile, 8)
        group = []
        for source, target in pairs:
            group.append((source.at[:, :, row, at, :], target.at[:, :, row, at, :]))
        for source, target in flats:
            group.append((source.at[:, row, at, :], target.at[:, row, at, :]))
        copies.append(
            [pltpu.make_async_copy(*ends_, sems.at[index, n]) for n, ends_ in enumerate(group)]
        )
        for copy in copies[-1]:
            copy.start()
    shift_copy.wait()
    for index, (row, tile) in enumerate(chunks):
        at = pl.ds(8 * tile, 8)
        for copy in copies[index]:
            copy.wait()
        groups = four(1 if tile == 0 else 0, shifts[0])
        for lanes in halves(depth):
            for slot in range(slots):
                code[slot, row, at, lanes] = jnp.where(
                    occupancy[slot, row, at, lanes] == 1, offsets[slot, row, at, lanes], GROUPS
                )
                for c in range(3):
                    rel[c, slot, row, at, lanes] = (
                        vel[c, slot, row, at, lanes] - thermal[c, slot, row, at, lanes]
                    )
            chunk_sums(pos, rel, code, value, geo, wsum, groups, row, at, lanes)

    def frame_of(*where):
        return {**geo_frame(geo, *where), **vel_frame(wsum, *where)}

    up, down = edges(frame_of, range(16), shifts[0], ends, cols)
    even = is_even("gy")
    for r in range(3):
        y_in[r] = jnp.where(even, up[r], down[r])
        y_out[r] = jnp.where(even, down[r], up[r])


def rest_sums_kernel(
    shifts, pos, rel, code, geo_near, wsum_near,
    geo, wsum, far, mid, near, value, low, high, part, shifted,
):
    _, rows, cols, depth = code.shape
    for row in range(rows):
        for tile in range(cols // 8):
            at = pl.ds(8 * tile, 8)
            by = 0 if tile == 0 else 1
            for o in four(1 - by, shifts[0]):
                for v in range(10):
                    geo[o, v, row, at, :] = geo_near[o, v, row, at, :]
                for v in range(6):
                    wsum[o, v, row, at, :] = wsum_near[o, v, row, at, :]
            groups = four(by, shifts[0])
            for lanes in halves(depth):
                chunk_sums(pos, rel, code, value, geo, wsum, groups, row, at, lanes)
    outs = (low, mid, high)
    expand(lambda *where: geo_frame(geo, *where), GEO, shifts[0], outs, None, None, part, shifted)
    expand(lambda *where: vel_frame(wsum, *where), VEL, shifts[0], outs, None, None, part, shifted)
    by_role(is_even("gx"), low, high, far, near)


def change_sums_kernel(step, pos, thermal, code, dsum, value):
    slots, rows, cols, depth = code.shape
    tiles = cols // 8

    def chunk(index, carry):
        row = index // tiles
        at = pl.ds(pl.multiple_of(8 * (index % tiles), 8), 8)
        for lanes in halves(depth):
            for slot in range(slots):
                p = [pos[c, slot, row, at, lanes] for c in range(3)]
                d = [
                    thermal[c, (slot + step) % slots, row, at, lanes]
                    - thermal[c, (slot + step + 1) % slots, row, at, lanes]
                    for c in range(3)
                ]
                for name, term in enumerate(d + cross(p, d)):
                    value[name, slot] = term
            codes = [code[slot, row, at, lanes] for slot in range(slots)]
            for base in (0, 4):

                def store(index, g, total):
                    dsum[base + g, index, row, at, lanes] = total

                accumulate(value, codes, range(base, base + 4), list(range(6)), store)
        return carry

    lax.fori_loop(0, rows * tiles, chunk, 0)


def roll(value, amount):
    return pltpu.roll(value, amount % value.shape[-1], value.ndim - 1)


GEO = (0, 1, 2, 3, 10, 11, 12, 13, 14, 15)
VEL = (4, 5, 6, 7, 8, 9)


def geo_frame(geo, o, frame, row, at):
    b = bits(frame)
    n = geo[o, 0, row, at, :]
    s = [geo[o, 1 + c, row, at, :] for c in range(3)]
    q = [s[c] + n if b[c] else s[c] for c in range(3)]
    out = {0: n, 1: q[0], 2: q[1], 3: q[2]}
    for k, (i, j) in enumerate(((0, 0), (1, 1), (2, 2), (0, 1), (0, 2), (1, 2))):
        value = geo[o, 4 + k, row, at, :]
        if b[i]:
            value = value + s[j]
        if b[j]:
            value = value + q[i]
        out[10 + k] = value
    return out


def vel_frame(wsum, o, frame, row, at):
    bx, by, bz = bits(frame)
    w = [wsum[o, c, row, at, :] for c in range(3)]
    l = [wsum[o, 3 + c, row, at, :] for c in range(3)]
    if bx:
        l = [l[0], l[1] - w[2], l[2] + w[1]]
    if by:
        l = [l[0] + w[2], l[1], l[2] - w[0]]
    if bz:
        l = [l[0] - w[1], l[1] + w[0], l[2]]
    return dict(zip(VEL, w + l))


def expand(frame_of, names, shift, rows, yup, ydn, part, shifted):
    cols = rows[0].shape[1]
    every = pl.ds(0, cols)
    for by in range(2):
        for bz in range(2):
            for bx in range(2):
                frame = 4 * bx + 2 * by + bz
                for row in range(2):
                    values = frame_of(frame ^ shift, frame, row, every)
                    for v in names:
                        if bx == 1 and row == 1:
                            part[by, bz, 1, v] += values[v]
                        else:
                            part[by, bz, row + 1 - bx, v] = values[v]
    for r in range(3):
        for v in names:
            near = part[0, 0, r, v] + roll(part[0, 1, r, v], -1)
            beyond = part[1, 0, r, v] + roll(part[1, 1, r, v], -1)
            shifted[r, v, cols:, :] = jnp.zeros((8, beyond.shape[1]), F32)
            shifted[r, v, :cols, :] = beyond
            main = near + shifted[r, v, 1 : cols + 1, :]
            rows[r][v] = main
            rows[r][16, v : v + 1, :] = beyond[0:1]
            if yup is not None:
                yup[r, v : v + 1, :] = main[cols - 1 : cols]
                ydn[r, v : v + 1, :] = beyond[0:1]


def edges(frame_of, names, shift, ends, cols):
    found = []
    for by, col in ((0, cols - 1), (1, 0)):
        for bz in range(2):
            for bx in range(2):
                frame = 4 * bx + 2 * by + bz
                for row in range(2):
                    own = frame_of(frame ^ shift, frame, row, pl.ds(col, 1))
                    for v in names:
                        if bx == 1 and row == 1:
                            ends[bz, 1, v : v + 1, :] += own[v]
                        else:
                            ends[bz, row + 1 - bx, v : v + 1, :] = own[v]
        found.append([ends[0, r] + roll(ends[1, r], -1) for r in range(3)])
    return found


def geometry_kernel(step, shifts, geo, row0, row1, row2, yup, ydn, part, shifted):
    outs = (row0, row1, row2)
    yup[...] = jnp.zeros_like(yup)
    ydn[...] = jnp.zeros_like(ydn)
    expand(
        lambda *where: geo_frame(geo, *where), GEO, shifts[step], outs, yup, ydn, part, shifted
    )


def by_role(even, first, second, one, two):
    for at in range(first.shape[0]):
        one[at] = jnp.where(even, first[at], second[at])
        two[at] = jnp.where(even, second[at], first[at])


def y_parts(y_in, y_out, r):
    even = is_even("gy")
    return jnp.where(even, y_out[r], y_in[r]), jnp.where(even, y_in[r], y_out[r])


def complete_row(row, low, high, out):
    last = out.shape[1] - 1
    out[...] = row[...]
    out[16] = row[16] + low
    for v in range(16):
        out[v, last : last + 1, :] = row[v, last : last + 1, :] + high[v : v + 1]


def fold_kernel(far, near, y_in, y_out, far_out, near_out):
    even = is_even("gx")
    low, high = y_parts(y_in, y_out, 0), y_parts(y_in, y_out, 2)
    far_ends = [jnp.where(even, low[at], high[at]) for at in range(2)]
    near_ends = [jnp.where(even, high[at], low[at]) for at in range(2)]
    complete_row(far, *far_ends, far_out)
    complete_row(near, *near_ends, near_out)


def solve(sums):
    inverse = 1.0 / jnp.maximum(sums[0], 1.0)
    first = sums[1:4]
    flow = sums[4:7]
    centre = [value * inverse for value in first]
    drift = [value * inverse for value in flow]
    moment = cross(centre, flow)
    torque = [sums[7 + c] - moment[c] for c in range(3)]
    mxx = sums[10] - first[0] * centre[0]
    myy = sums[11] - first[1] * centre[1]
    mzz = sums[12] - first[2] * centre[2]
    kxy = first[0] * centre[1] - sums[13]
    kxz = first[0] * centre[2] - sums[14]
    kyz = first[1] * centre[2] - sums[15]
    kxx = myy + mzz + RIDGE
    kyy = mxx + mzz + RIDGE
    kzz = mxx + myy + RIDGE
    adj_xx = kyy * kzz - kyz * kyz
    adj_yy = kxx * kzz - kxz * kxz
    adj_zz = kxx * kyy - kxy * kxy
    adj_xy = kxz * kyz - kxy * kzz
    adj_xz = kxy * kyz - kxz * kyy
    adj_yz = kxy * kxz - kxx * kyz
    scale = 1.0 / (kxx * adj_xx + kxy * adj_xy + kxz * adj_xz)
    spin = [
        (adj_xx * torque[0] + adj_xy * torque[1] + adj_xz * torque[2]) * scale,
        (adj_xy * torque[0] + adj_yy * torque[1] + adj_yz * torque[2]) * scale,
        (adj_xz * torque[0] + adj_yz * torque[1] + adj_zz * torque[2]) * scale,
    ]
    turned = cross(spin, centre)
    return [drift[c] - turned[c] for c in range(3)] + spin


def fill_table(own, around, table, total, which):
    far, mid, near = own
    y_in, y_out, x_far, x_near = around
    cols = (mid if far is None else far).shape[1]
    even = is_even("gx")
    if 1 in which:
        complete_row(mid, *y_parts(y_in, y_out, 1), total)
    for r in which:
        if r == 1:
            read = lambda v, at: total[v, at, :]
        else:
            mine = even if r == 0 else jnp.logical_not(even)
            read = lambda v, at: jnp.where(
                mine, far[v, at, :] + x_far[v, at, :], near[v, at, :] + x_near[v, at, :]
            )
        for t in range(cols // 8):
            at = pl.ds(8 * t, 8)
            state = solve([read(v, at) for v in range(16)])
            for v in range(6):
                table[0, v, r, 8 + 8 * t : 16 + 8 * t, :] = state[v]
                table[1, v, r, 8 + 8 * t : 16 + 8 * t, :] = roll(state[v], 1)
        state = solve([read(16, pl.ds(v, 1)) for v in range(16)])
        for v in range(6):
            wide = jnp.broadcast_to(state[v], (8, state[v].shape[1]))
            table[0, v, r, 0:8, :] = wide
            table[1, v, r, 0:8, :] = roll(wide, 1)


def shift_a(a, spin, b):
    a = list(a)
    if b[0]:
        a = [a[0], a[1] + spin[2], a[2] - spin[1]]
    if b[1]:
        a = [a[0] - spin[2], a[1], a[2] + spin[0]]
    if b[2]:
        a = [a[0] + spin[1], a[1] - spin[0], a[2]]
    return a


def update_groups(geo, dsum, shift, table, wsum, inner, done=None):
    cols = geo.shape[3]
    for code in range(GROUPS):
        bx, by, bz = bits(code)
        o = code ^ shift
        for row in range(2):
            if (bx == row) != inner:
                if done is not None:
                    for c in range(6):
                        wsum[o, c, row] = done[o, c, row]
                continue
            for t in range(cols // 8):
                at = pl.ds(8 * t, 8)
                from_col = 8 + 8 * t - by
                values = [table[bz, v, row + 1 - bx, from_col : from_col + 8, :] for v in range(6)]
                spin = values[3:]
                a = shift_a(values[:3], spin, (bx, by, bz))
                n = geo[o, 0, row, at, :]
                s = [geo[o, 1 + c, row, at, :] for c in range(3)]
                xx, yy, zz, xy, xz, yz = [geo[o, 4 + c, row, at, :] for c in range(6)]
                turn = cross(spin, s)
                arm = cross(s, a)
                own = [
                    (yy + zz) * spin[0] - xy * spin[1] - xz * spin[2],
                    (xx + zz) * spin[1] - xy * spin[0] - yz * spin[2],
                    (xx + yy) * spin[2] - xz * spin[0] - yz * spin[1],
                ]
                for c in range(3):
                    wsum[o, c, row, at, :] = dsum[o, c, row, at, :] + n * a[c] + turn[c]
                    wsum[o, 3 + c, row, at, :] = dsum[o, 3 + c, row, at, :] + arm[c] + own[c]


def step_kernel(
    step, shifts, geo, dsum, far, near, x_far, x_near, geoup, geodn, done,
    wsum, next_in, next_out, table, ends,
):
    cols = far.shape[1]
    fill_table((far, None, near), (None, None, x_far, x_near), table, None, (0, 2))
    update_groups(geo, dsum, shifts[step], table, wsum, False, done)
    for bz in range(2):
        for r in range(3):
            ends[bz, r] = jnp.zeros_like(ends[bz, r])
    up, down = edges(
        lambda *where: vel_frame(wsum, *where), VEL, shifts[step + 1], ends, cols
    )
    even = is_even("gy")
    for r in range(3):
        up_r, down_r = geoup[r] + up[r], geodn[r] + down[r]
        next_in[r] = jnp.where(even, up_r, down_r)
        next_out[r] = jnp.where(even, down_r, up_r)


def inner_step_kernel(step, shifts, geo, dsum, mid, y_in, y_out, wsum, total, table):
    fill_table((None, mid, None), (y_in, y_out, None, None), table, total, (1,))
    update_groups(geo, dsum, shifts[step], table, wsum, True)


def rows_kernel(
    step, shifts, wsum, geo0, geo1, geo2, far, mid, near, low, high, part, shifted
):
    rows = (low, mid, high)
    for target, source in zip(rows, (geo0, geo1, geo2)):
        for v in GEO:
            target[v] = source[v]
        target[16] = source[16]
    expand(
        lambda *where: vel_frame(wsum, *where), VEL, shifts[step + 1], rows, None, None, part, shifted
    )
    by_role(is_even("gx"), low, high, far, near)


def particle_block(shift, table, pos, thermal, code, variants, bx, row, tile, lanes, store):
    slots = code.shape[0]
    at = pl.ds(8 * tile, 8)
    for low in range(4):
        by, bz = low // 2, low % 2
        first = 8 + 8 * tile - by
        values = [table[bz, v, row + 1 - bx, first : first + 8, lanes] for v in range(6)]
        values[:3] = shift_a(values[:3], values[3:], (bx, by, bz))
        for v in range(6):
            variants[low, v] = values[v]
    for begin in range(0, slots, 4):
        block = range(begin, min(begin + 4, slots))
        base = [code[slot, row, at, lanes] for slot in block]
        k = [value ^ shift for value in base]
        isy = [(value & 2) != 0 for value in k]
        isz = [(value & 1) != 0 for value in k]
        state = [[] for _ in block]
        for v in range(6):
            four_ = [variants[low, v] for low in range(4)]
            for index in range(len(block)):
                lower = jnp.where(isy[index], four_[2], four_[0])
                upper = jnp.where(isy[index], four_[3], four_[1])
                state[index].append(jnp.where(isz[index], upper, lower))
        for index, slot in enumerate(block):
            mine = ((k[index] & 4) == 4 * bx) & (base[index] < GROUPS)
            turn = cross(state[index][3:], [pos[c, slot, row, at, lanes] for c in range(3)])
            hot = [thermal[c, (slot + STEPS - 1) % slots, row, at, lanes] for c in range(3)]
            store(slot, mine, [hot[c] + (state[index][c] + turn[c]) for c in range(3)])


def inner_particles_kernel(
    shifts, mid, y_in, y_out, pos, thermal, code, inner, total, table, variants
):
    _, rows, cols, depth = code.shape
    fill_table((None, mid, None), (y_in, y_out, None, None), table, total, (1,))
    for row in range(rows):
        for tile in range(cols // 8):
            at = pl.ds(8 * tile, 8)
            for lanes in halves(depth):

                def store(slot, mine, new):
                    for c in range(3):
                        inner[c, slot, row, at, lanes] = jnp.where(mine, new[c], 0.0)

                particle_block(
                    shifts[STEPS - 1], table, pos, thermal, code, variants, row, row, tile, lanes, store
                )


def particles_kernel(
    shifts, far, near, x_far, x_near, pos, thermal, code, inner,
    out, table, variants, fresh, sems,
):
    _, rows, cols, depth = code.shape
    fill_table((far, None, near), (None, None, x_far, x_near), table, None, (0, 2))
    copies = []
    for row in range(rows):
        for tile in range(cols // 8):
            at = pl.ds(8 * tile, 8)
            for lanes in halves(depth):

                def store(slot, mine, new):
                    for c in range(3):
                        fresh[c, slot, row, at, lanes] = jnp.where(
                            mine, new[c], inner[c, slot, row, at, lanes]
                        )

                particle_block(
                    shifts[STEPS - 1], table, pos, thermal, code, variants, 1 - row, row, tile, lanes,
                    store,
                )
            copy = pltpu.make_async_copy(
                fresh.at[:, :, row, at, :], out.at[:, :, row, at, :], sems.at[len(copies)]
            )
            copy.start()
            copies.append(copy)
    for copy in copies:
        copy.wait()


VMEM = pl.BlockSpec(memory_space=pltpu.VMEM)
SMEM = pl.BlockSpec(memory_space=pltpu.SMEM)
HBM = pl.BlockSpec(memory_space=pltpu.HBM)


def in_hbm(value):
    return pltpu.with_memory_space_constraint(value, pltpu.HBM)


def params(mib):
    return pltpu.CompilerParams(vmem_limit_bytes=mib * 2**20)


def shape(*dims):
    return jax.ShapeDtypeStruct(dims, F32)


def local(positions, velocities, thermal, offsets, occupancy, shift_codes):
    slots, rows, cols, depth = offsets.shape
    group_shape = lambda count: shape(GROUPS, count, rows, cols, depth)
    value = lambda count: pltpu.VMEM((count, slots, 8, 128), F32)
    vec_shape = shape(3, slots, rows, cols, depth)
    flat_shape = jax.ShapeDtypeStruct((slots, rows, cols, depth), jnp.int32)
    row_shape = shape(17, cols, depth)
    col_shape = shape(3, 16, depth)
    expand_out = [row_shape] * 3 + [col_shape] * 2
    expand_scratch = [
        pltpu.VMEM((2, 2, 3, 16, cols, depth), F32),
        pltpu.VMEM((3, 16, cols + 8, depth), F32),
    ]
    total = pltpu.VMEM((17, cols, depth), F32)
    table_shape = (2, 6, 3, cols + 8, depth)

    pos, hot, rel, code, geo_near, wsum_near, y_in, y_out = pl.pallas_call(
        near_sums_kernel,
        in_specs=[HBM] * 6,
        out_specs=[VMEM] * 8,
        out_shape=[vec_shape] * 3 + [flat_shape, group_shape(10), group_shape(6)] + [col_shape] * 2,
        scratch_shapes=[
            pltpu.VMEM(vec_shape.shape, F32),
            pltpu.VMEM(flat_shape.shape, jnp.int32),
            pltpu.VMEM(flat_shape.shape, jnp.int32),
            value(15),
            pltpu.VMEM((2, 3, 16, depth), F32),
            pltpu.SMEM((STEPS,), jnp.int32),
            pltpu.SemaphoreType.DMA((rows * cols // 8, 5)),
            pltpu.SemaphoreType.DMA,
        ],
        compiler_params=params(16),
        name="near_sums",
    )(*map(in_hbm, (shift_codes, positions, velocities, thermal, offsets, occupancy)))

    def swap(value, axis, odd):
        count = lax.axis_size(axis)
        partner = [(((i + odd) ^ 1) - odd) % count for i in range(count)]
        return lax.ppermute(value, axis, list(enumerate(partner)))

    def change_sums(step):
        return pl.pallas_call(
            functools.partial(change_sums_kernel, step),
            in_specs=[VMEM] * 3,
            out_specs=VMEM,
            out_shape=group_shape(6),
            scratch_shapes=[value(6)],
            compiler_params=params(8),
            name="change_sums",
        )(pos, hot, code)

    def geometry(step):
        return pl.pallas_call(
            functools.partial(geometry_kernel, step),
            in_specs=[SMEM, VMEM],
            out_specs=[VMEM] * 5,
            out_shape=expand_out,
            scratch_shapes=expand_scratch,
            compiler_params=params(12),
            name="geometry",
        )(shift_codes, geo)

    row_scratch = pltpu.VMEM(row_shape.shape, F32)

    for step in range(STEPS):
        got_out = swap(y_out, "gy", 1)
        got_in = swap(y_in, "gy", 0)
        if step == 0:
            geo, wsum, far, mid, near = pl.pallas_call(
                rest_sums_kernel,
                in_specs=[SMEM] + [VMEM] * 5,
                out_specs=[VMEM] * 5,
                out_shape=[group_shape(10), group_shape(6)] + [row_shape] * 3,
                scratch_shapes=[value(15), row_scratch, row_scratch] + expand_scratch,
                compiler_params=params(16),
                name="rest_sums",
            )(shift_codes, pos, rel, code, geo_near, wsum_near)
        else:
            far, mid, near = pl.pallas_call(
                functools.partial(rows_kernel, step - 1),
                in_specs=[SMEM] + [VMEM] * 4,
                out_specs=[VMEM] * 3,
                out_shape=[row_shape] * 3,
                scratch_shapes=[row_scratch, row_scratch] + expand_scratch,
                compiler_params=params(12),
                name="rows",
            )(shift_codes, wsum, *ahead)
        far, near = pl.pallas_call(
            fold_kernel,
            in_specs=[VMEM] * 4,
            out_specs=[VMEM] * 2,
            out_shape=[row_shape] * 2,
            compiler_params=params(2),
            name="fold",
        )(far, near, got_in, got_out)
        x_far = swap(far, "gx", 1)
        x_near = swap(near, "gx", 0)
        found = (far, near, x_far, x_near)
        inner_scratch = [total, pltpu.VMEM(table_shape, F32)]
        if step + 1 < STEPS:
            dsum = change_sums(step)
            *ahead, geoup, geodn = geometry(step + 1)
            done = pl.pallas_call(
                functools.partial(inner_step_kernel, step),
                in_specs=[SMEM] + [VMEM] * 5,
                out_specs=VMEM,
                out_shape=group_shape(6),
                scratch_shapes=inner_scratch,
                compiler_params=params(8),
                name="inner_step",
            )(shift_codes, geo, dsum, mid, got_in, got_out)
            wsum, y_in, y_out = pl.pallas_call(
                functools.partial(step_kernel, step),
                in_specs=[SMEM] + [VMEM] * 9,
                out_specs=[VMEM] * 3,
                out_shape=[group_shape(6)] + [col_shape] * 2,
                scratch_shapes=[pltpu.VMEM(table_shape, F32), pltpu.VMEM((2, 3, 16, depth), F32)],
                compiler_params=params(12),
                name="step",
            )(shift_codes, geo, dsum, *found, geoup, geodn, done)
        else:
            inner = pl.pallas_call(
                inner_particles_kernel,
                in_specs=[SMEM] + [VMEM] * 6,
                out_specs=VMEM,
                out_shape=vec_shape,
                scratch_shapes=inner_scratch + [pltpu.VMEM((4, 6, 8, 128), F32)],
                compiler_params=params(8),
                name="inner_particles",
            )(shift_codes, mid, got_in, got_out, pos, hot, code)

    return pl.pallas_call(
        particles_kernel,
        in_specs=[SMEM] + [VMEM] * 8,
        out_specs=HBM,
        out_shape=vec_shape,
        scratch_shapes=[
            pltpu.VMEM(table_shape, F32), pltpu.VMEM((4, 6, 8, 128), F32),
            pltpu.VMEM(vec_shape.shape, F32), pltpu.SemaphoreType.DMA((rows * cols // 8,)),
        ],
        compiler_params=params(12),
        name="particles",
    )(shift_codes, *found, pos, hot, code, inner)


def solution(mesh):
    in_specs = (
        P(None, None, "gx", "gy", None),
        P(None, None, "gx", "gy", None),
        P(None, None, "gx", "gy", None),
        P(None, "gx", "gy", None),
        P(None, "gx", "gy", None),
        P(),
    )
    out_specs = P(None, None, "gx", "gy", None)
    return jax.shard_map(local, mesh=mesh, in_specs=in_specs, out_specs=out_specs, check_vma=False)
```

```python
import functools

import jax
import jax.numpy as jnp
from jax import lax
from jax.experimental import pallas as pl
from jax.experimental.pallas import tpu as pltpu
from jax.sharding import PartitionSpec as P


STEPS = 3
RIDGE = 0.5
GROUPS = 8
F32 = jnp.float32


def bits(code):
    return code // 4, code // 2 % 2, code % 2


def is_even(axis):
    return lax.axis_index(axis) % 2 == 0


def cross(u, v):
    return [
        u[1] * v[2] - u[2] * v[1],
        u[2] * v[0] - u[0] * v[2],
        u[0] * v[1] - u[1] * v[0],
    ]


def accumulate(value_ref, codes, groups, names, store):
    sums = [[None] * len(groups) for _ in names]
    for slot, code in enumerate(codes):
        masks = [code == group for group in groups]
        for at, name in enumerate(names):
            value = 1.0 if name is None else value_ref[name, slot]
            for g, mask in enumerate(masks):
                part = jnp.where(mask, value, 0.0)
                old = sums[at][g]
                sums[at][g] = part if old is None else old + part
    for at in range(len(names)):
        for g in range(len(groups)):
            store(at, g, sums[at][g])


def moments(p, w):
    seconds = [p[0] * p[0], p[1] * p[1], p[2] * p[2], p[0] * p[1], p[0] * p[2], p[1] * p[2]]
    return p + seconds + w + cross(p, w)


def chunk_sums(pos, rel, code, value, geo, wsum, quads, row, at, lanes):
    slots = code.shape[0]
    for slot in range(slots):
        p = [pos[c, slot, row, at, lanes] for c in range(3)]
        w = [rel[c, slot, row, at, lanes] for c in range(3)]
        for name, term in enumerate(moments(p, w)):
            value[name, slot] = term
    codes = [code[slot, row, at, lanes] for slot in range(slots)]

    for groups in quads:

        def store_first(index, g, total):
            geo[groups[g], index, row, at, lanes] = total

        def store_second(index, g, total):
            if index < 2:
                geo[groups[g], 8 + index, row, at, lanes] = total
            else:
                wsum[groups[g], index - 2, row, at, lanes] = total

        accumulate(value, codes, groups, [None] + list(range(7)), store_first)
        accumulate(value, codes, groups, list(range(7, 15)), store_second)


def halves(depth):
    return [pl.ds(128 * half, 128) for half in range(depth // 128)]


def four(by, shift):
    return [(4 * bx + 2 * by + bz) ^ shift for bx in range(2) for bz in range(2)]


def near_sums_kernel(
    shifts_in, pos_in, vel_in, thermal_in, offsets_in, occupancy_in,
    pos, thermal, rel, code, geo, wsum, y_in, y_out,
    vel, offsets, occupancy, value, ends, shifts, sems, shift_sem,
):
    slots, rows, cols, depth = code.shape
    pairs = [(pos_in, pos), (vel_in, vel), (thermal_in, thermal)]
    flats = [(offsets_in, offsets), (occupancy_in, occupancy)]
    chunks = [(row, tile) for row in range(rows) for tile in range(cols // 8)]
    shift_copy = pltpu.make_async_copy(shifts_in, shifts, shift_sem)
    shift_copy.start()
    copies = []
    for index, (row, tile) in enumerate(chunks):
        at = pl.ds(8 * tile, 8)
        group = []
        for source, target in pairs:
            group.append((source.at[:, :, row, at, :], target.at[:, :, row, at, :]))
        for source, target in flats:
            group.append((source.at[:, row, at, :], target.at[:, row, at, :]))
        copies.append(
            [pltpu.make_async_copy(*ends_, sems.at[index, n]) for n, ends_ in enumerate(group)]
        )
        for copy in copies[-1]:
            copy.start()
    shift_copy.wait()
    for index, (row, tile) in enumerate(chunks):
        at = pl.ds(8 * tile, 8)
        for copy in copies[index]:
            copy.wait()
        bys = (1, 0) if index == 0 else ((1,) if tile == 0 else (0,))
        quads = [four(by, shifts[0]) for by in bys]
        for lanes in halves(depth):
            for slot in range(slots):
                code[slot, row, at, lanes] = jnp.where(
                    occupancy[slot, row, at, lanes] == 1, offsets[slot, row, at, lanes], GROUPS
                )
                for c in range(3):
                    rel[c, slot, row, at, lanes] = (
                        vel[c, slot, row, at, lanes] - thermal[c, slot, row, at, lanes]
                    )
            chunk_sums(pos, rel, code, value, geo, wsum, quads, row, at, lanes)

    def frame_of(*where):
        return {**geo_frame(geo, *where), **vel_frame(wsum, *where)}

    up, down = edges(frame_of, range(16), shifts[0], ends, cols)
    even = is_even("gy")
    for r in range(3):
        y_in[r] = jnp.where(even, up[r], down[r])
        y_out[r] = jnp.where(even, down[r], up[r])


def rest_sums_kernel(
    shifts, pos, rel, code, geo_near, wsum_near,
    geo, wsum, far, mid, near, value, low, high, part, shifted,
):
    _, rows, cols, depth = code.shape
    for row in range(rows):
        for tile in range(cols // 8):
            at = pl.ds(8 * tile, 8)
            by = 0 if tile == 0 else 1
            whole = row == 0 and tile == 0
            for o in range(GROUPS) if whole else four(1 - by, shifts[0]):
                for v in range(10):
                    geo[o, v, row, at, :] = geo_near[o, v, row, at, :]
                for v in range(6):
                    wsum[o, v, row, at, :] = wsum_near[o, v, row, at, :]
            if whole:
                continue
            quads = [four(by, shifts[0])]
            for lanes in halves(depth):
                chunk_sums(pos, rel, code, value, geo, wsum, quads, row, at, lanes)
    outs = (low, mid, high)
    expand(lambda *where: geo_frame(geo, *where), GEO, shifts[0], outs, None, None, part, shifted)
    expand(lambda *where: vel_frame(wsum, *where), VEL, shifts[0], outs, None, None, part, shifted)
    by_role(is_even("gx"), low, high, far, near)


def change_sums_kernel(step, pos, thermal, code, dsum, value):
    slots, rows, cols, depth = code.shape
    tiles = cols // 8

    def chunk(index, carry):
        row = index // tiles
        at = pl.ds(pl.multiple_of(8 * (index % tiles), 8), 8)
        for lanes in halves(depth):
            for slot in range(slots):
                p = [pos[c, slot, row, at, lanes] for c in range(3)]
                d = [
                    thermal[c, (slot + step) % slots, row, at, lanes]
                    - thermal[c, (slot + step + 1) % slots, row, at, lanes]
                    for c in range(3)
                ]
                for name, term in enumerate(d + cross(p, d)):
                    value[name, slot] = term
            codes = [code[slot, row, at, lanes] for slot in range(slots)]
            for base in (0, 4):

                def store(index, g, total):
                    dsum[base + g, index, row, at, lanes] = total

                accumulate(value, codes, range(base, base + 4), list(range(6)), store)
        return carry

    lax.fori_loop(0, rows * tiles, chunk, 0)


def roll(value, amount):
    return pltpu.roll(value, amount % value.shape[-1], value.ndim - 1)


GEO = (0, 1, 2, 3, 10, 11, 12, 13, 14, 15)
VEL = (4, 5, 6, 7, 8, 9)


def geo_frame(geo, o, frame, row, at):
    b = bits(frame)
    n = geo[o, 0, row, at, :]
    s = [geo[o, 1 + c, row, at, :] for c in range(3)]
    q = [s[c] + n if b[c] else s[c] for c in range(3)]
    out = {0: n, 1: q[0], 2: q[1], 3: q[2]}
    for k, (i, j) in enumerate(((0, 0), (1, 1), (2, 2), (0, 1), (0, 2), (1, 2))):
        value = geo[o, 4 + k, row, at, :]
        if b[i]:
            value = value + s[j]
        if b[j]:
            value = value + q[i]
        out[10 + k] = value
    return out


def vel_frame(wsum, o, frame, row, at):
    bx, by, bz = bits(frame)
    w = [wsum[o, c, row, at, :] for c in range(3)]
    l = [wsum[o, 3 + c, row, at, :] for c in range(3)]
    if bx:
        l = [l[0], l[1] - w[2], l[2] + w[1]]
    if by:
        l = [l[0] + w[2], l[1], l[2] - w[0]]
    if bz:
        l = [l[0] - w[1], l[1] + w[0], l[2]]
    return dict(zip(VEL, w + l))


def expand(frame_of, names, shift, rows, yup, ydn, part, shifted):
    cols = rows[0].shape[1]
    every = pl.ds(0, cols)
    for by in range(2):
        for bz in range(2):
            for bx in range(2):
                frame = 4 * bx + 2 * by + bz
                for row in range(2):
                    values = frame_of(frame ^ shift, frame, row, every)
                    for v in names:
                        if bx == 1 and row == 1:
                            part[by, bz, 1, v] += values[v]
                        else:
                            part[by, bz, row + 1 - bx, v] = values[v]
    for r in range(3):
        for v in names:
            near = part[0, 0, r, v] + roll(part[0, 1, r, v], -1)
            beyond = part[1, 0, r, v] + roll(part[1, 1, r, v], -1)
            shifted[r, v, cols:, :] = jnp.zeros((8, beyond.shape[1]), F32)
            shifted[r, v, :cols, :] = beyond
            main = near + shifted[r, v, 1 : cols + 1, :]
            rows[r][v] = main
            rows[r][16, v : v + 1, :] = beyond[0:1]
            if yup is not None:
                yup[r, v : v + 1, :] = main[cols - 1 : cols]
                ydn[r, v : v + 1, :] = beyond[0:1]


def edges(frame_of, names, shift, ends, cols):
    found = []
    for by, col in ((0, cols - 1), (1, 0)):
        for bz in range(2):
            for bx in range(2):
                frame = 4 * bx + 2 * by + bz
                for row in range(2):
                    own = frame_of(frame ^ shift, frame, row, pl.ds(col, 1))
                    for v in names:
                        if bx == 1 and row == 1:
                            ends[bz, 1, v : v + 1, :] += own[v]
                        else:
                            ends[bz, row + 1 - bx, v : v + 1, :] = own[v]
        found.append([ends[0, r] + roll(ends[1, r], -1) for r in range(3)])
    return found


def geometry_kernel(step, shifts, geo, row0, row1, row2, yup, ydn, part, shifted):
    outs = (row0, row1, row2)
    yup[...] = jnp.zeros_like(yup)
    ydn[...] = jnp.zeros_like(ydn)
    expand(
        lambda *where: geo_frame(geo, *where), GEO, shifts[step], outs, yup, ydn, part, shifted
    )


def by_role(even, first, second, one, two):
    for at in range(first.shape[0]):
        one[at] = jnp.where(even, first[at], second[at])
        two[at] = jnp.where(even, second[at], first[at])


def y_parts(y_in, y_out, r):
    even = is_even("gy")
    return jnp.where(even, y_out[r], y_in[r]), jnp.where(even, y_in[r], y_out[r])


def complete_row(row, low, high, out):
    last = out.shape[1] - 1
    out[...] = row[...]
    out[16] = row[16] + low
    for v in range(16):
        out[v, last : last + 1, :] = row[v, last : last + 1, :] + high[v : v + 1]


def fold_kernel(far, near, y_in, y_out, far_out, near_out):
    even = is_even("gx")
    low, high = y_parts(y_in, y_out, 0), y_parts(y_in, y_out, 2)
    far_ends = [jnp.where(even, low[at], high[at]) for at in range(2)]
    near_ends = [jnp.where(even, high[at], low[at]) for at in range(2)]
    complete_row(far, *far_ends, far_out)
    complete_row(near, *near_ends, near_out)


def solve(sums):
    inverse = 1.0 / jnp.maximum(sums[0], 1.0)
    first = sums[1:4]
    flow = sums[4:7]
    centre = [value * inverse for value in first]
    drift = [value * inverse for value in flow]
    moment = cross(centre, flow)
    torque = [sums[7 + c] - moment[c] for c in range(3)]
    mxx = sums[10] - first[0] * centre[0]
    myy = sums[11] - first[1] * centre[1]
    mzz = sums[12] - first[2] * centre[2]
    kxy = first[0] * centre[1] - sums[13]
    kxz = first[0] * centre[2] - sums[14]
    kyz = first[1] * centre[2] - sums[15]
    kxx = myy + mzz + RIDGE
    kyy = mxx + mzz + RIDGE
    kzz = mxx + myy + RIDGE
    adj_xx = kyy * kzz - kyz * kyz
    adj_yy = kxx * kzz - kxz * kxz
    adj_zz = kxx * kyy - kxy * kxy
    adj_xy = kxz * kyz - kxy * kzz
    adj_xz = kxy * kyz - kxz * kyy
    adj_yz = kxy * kxz - kxx * kyz
    scale = 1.0 / (kxx * adj_xx + kxy * adj_xy + kxz * adj_xz)
    spin = [
        (adj_xx * torque[0] + adj_xy * torque[1] + adj_xz * torque[2]) * scale,
        (adj_xy * torque[0] + adj_yy * torque[1] + adj_yz * torque[2]) * scale,
        (adj_xz * torque[0] + adj_yz * torque[1] + adj_zz * torque[2]) * scale,
    ]
    turned = cross(spin, centre)
    return [drift[c] - turned[c] for c in range(3)] + spin


def fill_table(own, around, table, total, which):
    far, mid, near = own
    y_in, y_out, x_far, x_near = around
    cols = (mid if far is None else far).shape[1]
    even = is_even("gx")
    if 1 in which:
        complete_row(mid, *y_parts(y_in, y_out, 1), total)
    for r in which:
        if r == 1:
            read = lambda v, at: total[v, at, :]
        else:
            mine = even if r == 0 else jnp.logical_not(even)
            read = lambda v, at: jnp.where(
                mine, far[v, at, :] + x_far[v, at, :], near[v, at, :] + x_near[v, at, :]
            )
        for t in range(cols // 8):
            at = pl.ds(8 * t, 8)
            state = solve([read(v, at) for v in range(16)])
            for v in range(6):
                table[0, v, r, 8 + 8 * t : 16 + 8 * t, :] = state[v]
                table[1, v, r, 8 + 8 * t : 16 + 8 * t, :] = roll(state[v], 1)
        state = solve([read(16, pl.ds(v, 1)) for v in range(16)])
        for v in range(6):
            wide = jnp.broadcast_to(state[v], (8, state[v].shape[1]))
            table[0, v, r, 0:8, :] = wide
            table[1, v, r, 0:8, :] = roll(wide, 1)


def shift_a(a, spin, b):
    a = list(a)
    if b[0]:
        a = [a[0], a[1] + spin[2], a[2] - spin[1]]
    if b[1]:
        a = [a[0] - spin[2], a[1], a[2] + spin[0]]
    if b[2]:
        a = [a[0] + spin[1], a[1] - spin[0], a[2]]
    return a


def update_groups(geo, dsum, shift, table, wsum, inner, done=None):
    cols = geo.shape[3]
    for code in range(GROUPS):
        bx, by, bz = bits(code)
        o = code ^ shift
        for row in range(2):
            if (bx == row) != inner:
                if done is not None:
                    for c in range(6):
                        wsum[o, c, row] = done[o, c, row]
                continue
            for t in range(cols // 8):
                at = pl.ds(8 * t, 8)
                from_col = 8 + 8 * t - by
                values = [table[bz, v, row + 1 - bx, from_col : from_col + 8, :] for v in range(6)]
                spin = values[3:]
                a = shift_a(values[:3], spin, (bx, by, bz))
                n = geo[o, 0, row, at, :]
                s = [geo[o, 1 + c, row, at, :] for c in range(3)]
                xx, yy, zz, xy, xz, yz = [geo[o, 4 + c, row, at, :] for c in range(6)]
                turn = cross(spin, s)
                arm = cross(s, a)
                own = [
                    (yy + zz) * spin[0] - xy * spin[1] - xz * spin[2],
                    (xx + zz) * spin[1] - xy * spin[0] - yz * spin[2],
                    (xx + yy) * spin[2] - xz * spin[0] - yz * spin[1],
                ]
                for c in range(3):
                    wsum[o, c, row, at, :] = dsum[o, c, row, at, :] + n * a[c] + turn[c]
                    wsum[o, 3 + c, row, at, :] = dsum[o, 3 + c, row, at, :] + arm[c] + own[c]


def step_kernel(
    step, shifts, geo, dsum, far, near, x_far, x_near, geoup, geodn, done,
    wsum, next_in, next_out, table, ends,
):
    cols = far.shape[1]
    fill_table((far, None, near), (None, None, x_far, x_near), table, None, (0, 2))
    update_groups(geo, dsum, shifts[step], table, wsum, False, done)
    for bz in range(2):
        for r in range(3):
            ends[bz, r] = jnp.zeros_like(ends[bz, r])
    up, down = edges(
        lambda *where: vel_frame(wsum, *where), VEL, shifts[step + 1], ends, cols
    )
    even = is_even("gy")
    for r in range(3):
        up_r, down_r = geoup[r] + up[r], geodn[r] + down[r]
        next_in[r] = jnp.where(even, up_r, down_r)
        next_out[r] = jnp.where(even, down_r, up_r)


def inner_step_kernel(step, shifts, geo, dsum, mid, y_in, y_out, wsum, total, table):
    fill_table((None, mid, None), (y_in, y_out, None, None), table, total, (1,))
    update_groups(geo, dsum, shifts[step], table, wsum, True)


def rows_kernel(
    step, shifts, wsum, geo0, geo1, geo2, far, mid, near, low, high, part, shifted
):
    rows = (low, mid, high)
    for target, source in zip(rows, (geo0, geo1, geo2)):
        for v in GEO:
            target[v] = source[v]
        target[16] = source[16]
    expand(
        lambda *where: vel_frame(wsum, *where), VEL, shifts[step + 1], rows, None, None, part, shifted
    )
    by_role(is_even("gx"), low, high, far, near)


def particle_block(shift, table, pos, thermal, code, variants, bx, row, tile, lanes, store):
    slots = code.shape[0]
    at = pl.ds(8 * tile, 8)
    for low in range(4):
        by, bz = low // 2, low % 2
        first = 8 + 8 * tile - by
        values = [table[bz, v, row + 1 - bx, first : first + 8, lanes] for v in range(6)]
        values[:3] = shift_a(values[:3], values[3:], (bx, by, bz))
        for v in range(6):
            variants[low, v] = values[v]
    for begin in range(0, slots, 4):
        block = range(begin, min(begin + 4, slots))
        base = [code[slot, row, at, lanes] for slot in block]
        k = [value ^ shift for value in base]
        isy = [(value & 2) != 0 for value in k]
        isz = [(value & 1) != 0 for value in k]
        state = [[] for _ in block]
        for v in range(6):
            four_ = [variants[low, v] for low in range(4)]
            for index in range(len(block)):
                lower = jnp.where(isy[index], four_[2], four_[0])
                upper = jnp.where(isy[index], four_[3], four_[1])
                state[index].append(jnp.where(isz[index], upper, lower))
        for index, slot in enumerate(block):
            mine = ((k[index] & 4) == 4 * bx) & (base[index] < GROUPS)
            turn = cross(state[index][3:], [pos[c, slot, row, at, lanes] for c in range(3)])
            hot = [thermal[c, (slot + STEPS - 1) % slots, row, at, lanes] for c in range(3)]
            store(slot, mine, [hot[c] + (state[index][c] + turn[c]) for c in range(3)])


def inner_particles_kernel(
    shifts, mid, y_in, y_out, pos, thermal, code, inner, total, table, variants
):
    _, rows, cols, depth = code.shape
    fill_table((None, mid, None), (y_in, y_out, None, None), table, total, (1,))
    for row in range(rows):
        for tile in range(cols // 8):
            at = pl.ds(8 * tile, 8)
            for lanes in halves(depth):

                def store(slot, mine, new):
                    for c in range(3):
                        inner[c, slot, row, at, lanes] = jnp.where(mine, new[c], 0.0)

                particle_block(
                    shifts[STEPS - 1], table, pos, thermal, code, variants, row, row, tile, lanes, store
                )


def particles_kernel(
    shifts, far, near, x_far, x_near, pos, thermal, code, inner,
    out, table, variants, fresh, sems,
):
    _, rows, cols, depth = code.shape
    fill_table((far, None, near), (None, None, x_far, x_near), table, None, (0, 2))
    copies = []
    for row in range(rows):
        for tile in range(cols // 8):
            at = pl.ds(8 * tile, 8)
            for lanes in halves(depth):

                def store(slot, mine, new):
                    for c in range(3):
                        fresh[c, slot, row, at, lanes] = jnp.where(
                            mine, new[c], inner[c, slot, row, at, lanes]
                        )

                particle_block(
                    shifts[STEPS - 1], table, pos, thermal, code, variants, 1 - row, row, tile, lanes,
                    store,
                )
            copy = pltpu.make_async_copy(
                fresh.at[:, :, row, at, :], out.at[:, :, row, at, :], sems.at[len(copies)]
            )
            copy.start()
            copies.append(copy)
    for copy in copies:
        copy.wait()


VMEM = pl.BlockSpec(memory_space=pltpu.VMEM)
SMEM = pl.BlockSpec(memory_space=pltpu.SMEM)
HBM = pl.BlockSpec(memory_space=pltpu.HBM)


def in_hbm(value):
    return pltpu.with_memory_space_constraint(value, pltpu.HBM)


def params(mib):
    return pltpu.CompilerParams(vmem_limit_bytes=mib * 2**20)


def shape(*dims):
    return jax.ShapeDtypeStruct(dims, F32)


def local(positions, velocities, thermal, offsets, occupancy, shift_codes):
    slots, rows, cols, depth = offsets.shape
    group_shape = lambda count: shape(GROUPS, count, rows, cols, depth)
    value = lambda count: pltpu.VMEM((count, slots, 8, 128), F32)
    vec_shape = shape(3, slots, rows, cols, depth)
    flat_shape = jax.ShapeDtypeStruct((slots, rows, cols, depth), jnp.int32)
    row_shape = shape(17, cols, depth)
    col_shape = shape(3, 16, depth)
    expand_out = [row_shape] * 3 + [col_shape] * 2
    expand_scratch = [
        pltpu.VMEM((2, 2, 3, 16, cols, depth), F32),
        pltpu.VMEM((3, 16, cols + 8, depth), F32),
    ]
    total = pltpu.VMEM((17, cols, depth), F32)
    table_shape = (2, 6, 3, cols + 8, depth)

    pos, hot, rel, code, geo_near, wsum_near, y_in, y_out = pl.pallas_call(
        near_sums_kernel,
        in_specs=[HBM] * 6,
        out_specs=[VMEM] * 8,
        out_shape=[vec_shape] * 3 + [flat_shape, group_shape(10), group_shape(6)] + [col_shape] * 2,
        scratch_shapes=[
            pltpu.VMEM(vec_shape.shape, F32),
            pltpu.VMEM(flat_shape.shape, jnp.int32),
            pltpu.VMEM(flat_shape.shape, jnp.int32),
            value(15),
            pltpu.VMEM((2, 3, 16, depth), F32),
            pltpu.SMEM((STEPS,), jnp.int32),
            pltpu.SemaphoreType.DMA((rows * cols // 8, 5)),
            pltpu.SemaphoreType.DMA,
        ],
        compiler_params=params(16),
        name="near_sums",
    )(*map(in_hbm, (shift_codes, positions, velocities, thermal, offsets, occupancy)))

    def swap(value, axis, odd):
        count = lax.axis_size(axis)
        partner = [(((i + odd) ^ 1) - odd) % count for i in range(count)]
        return lax.ppermute(value, axis, list(enumerate(partner)))

    def change_sums(step):
        return pl.pallas_call(
            functools.partial(change_sums_kernel, step),
            in_specs=[VMEM] * 3,
            out_specs=VMEM,
            out_shape=group_shape(6),
            scratch_shapes=[value(6)],
            compiler_params=params(8),
            name="change_sums",
        )(pos, hot, code)

    def geometry(step):
        return pl.pallas_call(
            functools.partial(geometry_kernel, step),
            in_specs=[SMEM, VMEM],
            out_specs=[VMEM] * 5,
            out_shape=expand_out,
            scratch_shapes=expand_scratch,
            compiler_params=params(12),
            name="geometry",
        )(shift_codes, geo)

    row_scratch = pltpu.VMEM(row_shape.shape, F32)

    for step in range(STEPS):
        got_out = swap(y_out, "gy", 1)
        got_in = swap(y_in, "gy", 0)
        if step == 0:
            geo, wsum, far, mid, near = pl.pallas_call(
                rest_sums_kernel,
                in_specs=[SMEM] + [VMEM] * 5,
                out_specs=[VMEM] * 5,
                out_shape=[group_shape(10), group_shape(6)] + [row_shape] * 3,
                scratch_shapes=[value(15), row_scratch, row_scratch] + expand_scratch,
                compiler_params=params(16),
                name="rest_sums",
            )(shift_codes, pos, rel, code, geo_near, wsum_near)
        else:
            far, mid, near = pl.pallas_call(
                functools.partial(rows_kernel, step - 1),
                in_specs=[SMEM] + [VMEM] * 4,
                out_specs=[VMEM] * 3,
                out_shape=[row_shape] * 3,
                scratch_shapes=[row_scratch, row_scratch] + expand_scratch,
                compiler_params=params(12),
                name="rows",
            )(shift_codes, wsum, *ahead)
        far, near = pl.pallas_call(
            fold_kernel,
            in_specs=[VMEM] * 4,
            out_specs=[VMEM] * 2,
            out_shape=[row_shape] * 2,
            compiler_params=params(2),
            name="fold",
        )(far, near, got_in, got_out)
        x_far = swap(far, "gx", 1)
        x_near = swap(near, "gx", 0)
        found = (far, near, x_far, x_near)
        inner_scratch = [total, pltpu.VMEM(table_shape, F32)]
        if step + 1 < STEPS:
            dsum = change_sums(step)
            *ahead, geoup, geodn = geometry(step + 1)
            done = pl.pallas_call(
                functools.partial(inner_step_kernel, step),
                in_specs=[SMEM] + [VMEM] * 5,
                out_specs=VMEM,
                out_shape=group_shape(6),
                scratch_shapes=inner_scratch,
                compiler_params=params(8),
                name="inner_step",
            )(shift_codes, geo, dsum, mid, got_in, got_out)
            wsum, y_in, y_out = pl.pallas_call(
                functools.partial(step_kernel, step),
                in_specs=[SMEM] + [VMEM] * 9,
                out_specs=[VMEM] * 3,
                out_shape=[group_shape(6)] + [col_shape] * 2,
                scratch_shapes=[pltpu.VMEM(table_shape, F32), pltpu.VMEM((2, 3, 16, depth), F32)],
                compiler_params=params(12),
                name="step",
            )(shift_codes, geo, dsum, *found, geoup, geodn, done)
        else:
            inner = pl.pallas_call(
                inner_particles_kernel,
                in_specs=[SMEM] + [VMEM] * 6,
                out_specs=VMEM,
                out_shape=vec_shape,
                scratch_shapes=inner_scratch + [pltpu.VMEM((4, 6, 8, 128), F32)],
                compiler_params=params(8),
                name="inner_particles",
            )(shift_codes, mid, got_in, got_out, pos, hot, code)

    return pl.pallas_call(
        particles_kernel,
        in_specs=[SMEM] + [VMEM] * 8,
        out_specs=HBM,
        out_shape=vec_shape,
        scratch_shapes=[
            pltpu.VMEM(table_shape, F32), pltpu.VMEM((4, 6, 8, 128), F32),
            pltpu.VMEM(vec_shape.shape, F32), pltpu.SemaphoreType.DMA((rows * cols // 8,)),
        ],
        compiler_params=params(12),
        name="particles",
    )(shift_codes, *found, pos, hot, code, inner)


def solution(mesh):
    in_specs = (
        P(None, None, "gx", "gy", None),
        P(None, None, "gx", "gy", None),
        P(None, None, "gx", "gy", None),
        P(None, "gx", "gy", None),
        P(None, "gx", "gy", None),
        P(),
    )
    out_specs = P(None, None, "gx", "gy", None)
    return jax.shard_map(local, mesh=mesh, in_specs=in_specs, out_specs=out_specs, check_vma=False)
```
